256 devices in a mesh: g: 256 (over z, y, x, core).
Axes of the slice: x: 4, y: 4, z: 8, core: 2. Of those that a mesh axis runs over, the one named last changes fastest.
Arguments:
- x_store: bfloat16 [524288, 602], P('g')
- frontier_ids: int32 [524288], P('g')
- nbr_one: int32 [131072, 25], P('g')
- nbr_two: int32 [16384, 10], P('g')
- labels: int32 [16384], P('g')
- w_self1: bfloat16 [602, 256], replicated
- w_nbr1: bfloat16 [602, 256], replicated
- w_self2: bfloat16 [256, 41], replicated
- w_nbr2: bfloat16 [256, 41], replicated
Outputs:
- output 1: float32 [], replicated
- output 2: float32 [602, 256], replicated
- output 3: float32 [602, 256], replicated
- output 4: float32 [256, 41], replicated
- output 5: float32 [256, 41], replicated
All inputs are finite; a program needn't handle non-finite values.
Results may differ from the reference program's by a relative error of at most 0.00261.
Values are sent between devices in bfloat16 or wider.
A program may use at most 768 MiB of HBM per device.

```python
import jax
import jax.numpy as jnp
from jax import lax

GROUP = 256
FEATURES = 602
HIDDEN = 256
CLASSES = 41
FANOUT_ONE = 25
FANOUT_TWO = 10
SEEDS_DEV = 64
STORE_ROWS = 2048

TARGETS_ONE = 8 * SEEDS_DEV
FRONTIER = 32 * SEEDS_DEV
HALO = FRONTIER // 32


def permute_positions(one_key):
    return jax.random.permutation(one_key, FRONTIER - SEEDS_DEV).astype(jnp.int32)


def draw_frontier(root_key):
    key_count, key_rank, key_offset = jax.random.split(root_key, 3)
    cross_counts = jax.random.randint(key_count, (2, GROUP), HALO // 2, HALO + 1, jnp.int32)
    cross_counts = cross_counts.at[:, 0].set(HALO)
    pos_rank = jax.vmap(permute_positions)(jax.random.split(key_rank, GROUP))
    seed_rank = jnp.full((GROUP, SEEDS_DEV), FRONTIER, jnp.int32)
    pos_rank = jnp.concatenate([seed_rank, pos_rank], axis=1)
    left_count = cross_counts[0][:, None]
    right_end = left_count + cross_counts[1][:, None]
    block_ids = jnp.arange(GROUP, dtype=jnp.int32)[:, None]
    owner_shard = jnp.where(pos_rank < left_count, (block_ids - 1) % GROUP,
                            jnp.where(pos_rank < right_end, (block_ids + 1) % GROUP, block_ids))
    row_offset = jax.random.randint(key_offset, (GROUP, FRONTIER), 0, STORE_ROWS, jnp.int32)
    return (owner_shard * STORE_ROWS + row_offset).reshape(-1).astype(jnp.int32)


def setup_inputs(seed: int = 0) -> dict:
    root_key = jax.random.key(seed)
    key_list = jax.random.split(root_key, 9)
    x_store = jax.random.normal(key_list[0], (GROUP * STORE_ROWS, FEATURES), jnp.float32).astype(jnp.bfloat16)
    frontier_ids = draw_frontier(key_list[1])
    nbr_one = jax.random.randint(key_list[2], (GROUP * TARGETS_ONE, FANOUT_ONE), 0, FRONTIER, jnp.int32)
    nbr_two = jax.random.randint(key_list[3], (GROUP * SEEDS_DEV, FANOUT_TWO), 0, TARGETS_ONE, jnp.int32)
    labels = jax.random.randint(key_list[4], (GROUP * SEEDS_DEV,), 0, CLASSES, jnp.int32)
    w_self1 = (jax.random.normal(key_list[5], (FEATURES, HIDDEN), jnp.float32) * (2.0 * FEATURES) ** -0.5).astype(jnp.bfloat16)
    w_nbr1 = (jax.random.normal(key_list[6], (FEATURES, HIDDEN), jnp.float32) * (2.0 * FEATURES / FANOUT_ONE) ** -0.5).astype(jnp.bfloat16)
    w_self2 = (jax.random.normal(key_list[7], (HIDDEN, CLASSES), jnp.float32) * HIDDEN ** -0.5).astype(jnp.bfloat16)
    w_nbr2 = (jax.random.normal(key_list[8], (HIDDEN, CLASSES), jnp.float32) * HIDDEN ** -0.5).astype(jnp.bfloat16)
    return {'x_store': x_store, 'frontier_ids': frontier_ids, 'nbr_one': nbr_one, 'nbr_two': nbr_two,
            'labels': labels, 'w_self1': w_self1, 'w_nbr1': w_nbr1, 'w_self2': w_self2, 'w_nbr2': w_nbr2}


def block_step(x_store, w_self1, w_nbr1, w_self2, w_nbr2, block_in):
    front_ids, nbr_one, nbr_two, labels = block_in
    x_front = x_store[front_ids]
    agg_one = (jnp.sum(x_front[nbr_one].astype(jnp.float32), axis=1) / FANOUT_ONE).astype(jnp.bfloat16)
    x_target = x_front[:TARGETS_ONE]
    z_one = (jnp.dot(x_target, w_self1, preferred_element_type=jnp.float32)
             + jnp.dot(agg_one, w_nbr1, preferred_element_type=jnp.float32))
    h_one = jnp.maximum(z_one, 0.0).astype(jnp.bfloat16)
    agg_two = (jnp.sum(h_one[nbr_two].astype(jnp.float32), axis=1) / FANOUT_TWO).astype(jnp.bfloat16)
    h_seed = h_one[:SEEDS_DEV]
    logits = (jnp.dot(h_seed, w_self2, preferred_element_type=jnp.float32)
              + jnp.dot(agg_two, w_nbr2, preferred_element_type=jnp.float32))
    log_prob = jax.nn.log_softmax(logits, axis=-1)
    one_hot = (labels[:, None] == jnp.arange(CLASSES, dtype=jnp.int32)[None, :]).astype(jnp.float32)
    loss_sum = -jnp.sum(one_hot * log_prob)
    grad_logits = ((jnp.exp(log_prob) - one_hot) / (GROUP * SEEDS_DEV)).astype(jnp.bfloat16)
    grad_self2 = jnp.dot(h_seed.T, grad_logits, preferred_element_type=jnp.float32)
    grad_nbr2 = jnp.dot(agg_two.T, grad_logits, preferred_element_type=jnp.float32)
    grad_seed = jnp.dot(grad_logits, w_self2.T, preferred_element_type=jnp.float32)
    grad_agg = jnp.dot(grad_logits, w_nbr2.T, preferred_element_type=jnp.float32) / FANOUT_TWO
    spread = jnp.broadcast_to(grad_agg[:, None, :], (SEEDS_DEV, FANOUT_TWO, HIDDEN)).reshape(SEEDS_DEV * FANOUT_TWO, HIDDEN)
    row_ids = jnp.concatenate([nbr_two.reshape(-1), jnp.arange(SEEDS_DEV, dtype=jnp.int32)])
    grad_h = jax.ops.segment_sum(jnp.concatenate([spread, grad_seed], axis=0), row_ids, num_segments=TARGETS_ONE)
    grad_z = jnp.where(z_one > 0, grad_h, 0.0).astype(jnp.bfloat16)
    grad_self1 = jnp.dot(x_target.T, grad_z, preferred_element_type=jnp.float32)
    grad_nbr1 = jnp.dot(agg_one.T, grad_z, preferred_element_type=jnp.float32)
    return loss_sum, grad_self1, grad_nbr1, grad_self2, grad_nbr2


def reference(x_store, frontier_ids, nbr_one, nbr_two, labels, w_self1, w_nbr1, w_self2, w_nbr2):
    block_inputs = (frontier_ids.reshape(GROUP, FRONTIER),
                    nbr_one.reshape(GROUP, TARGETS_ONE, FANOUT_ONE),
                    nbr_two.reshape(GROUP, SEEDS_DEV, FANOUT_TWO),
                    labels.reshape(GROUP, SEEDS_DEV))

    def scan_step(running, block_in):
        fresh_vals = block_step(x_store, w_self1, w_nbr1, w_self2, w_nbr2, block_in)
        return tuple(old_val + new_val for old_val, new_val in zip(running, fresh_vals)), None

    start_sums = (jnp.zeros((), jnp.float32),
                  jnp.zeros((FEATURES, HIDDEN), jnp.float32),
                  jnp.zeros((FEATURES, HIDDEN), jnp.float32),
                  jnp.zeros((HIDDEN, CLASSES), jnp.float32),
                  jnp.zeros((HIDDEN, CLASSES), jnp.float32))
    totals, _ = lax.scan(scan_step, start_sums, block_inputs)
    return (totals[0] / (GROUP * SEEDS_DEV), totals[1], totals[2], totals[3], totals[4])
```

```python
import functools

import jax
import jax.numpy as jnp
from jax import lax
from jax.experimental import pallas as pl
from jax.experimental.pallas import tpu as pltpu
from jax.sharding import PartitionSpec as P

MESH = pl.DeviceIdType.MESH
F32, BF16, I32 = jnp.float32, jnp.bfloat16, jnp.int32
VMEM = pltpu.VMEM

HALO = 64
FIELDS, FIELD_BITS = 6, 5
CHUNK_A, CHUNK_B = 6, 5


def dims_of(group):
    return {256: (4, 4, 8), 16: (2, 2, 2)}[group]


def dot(a, b, ca=1, cb=0):
    return lax.dot_general(a, b, (((ca,), (cb,)), ((), ())), preferred_element_type=F32)


def iota(shape, dim):
    return lax.broadcasted_iota(I32, shape, dim)


def frontier_ext(fid, me, group, rows_log2):
    store = 1 << rows_log2
    owner = lax.shift_right_logical(fid, rows_log2)
    off = lax.bitwise_and(fid, store - 1)
    left, right = lax.rem(me + group - 1, group), lax.rem(me + 1, group)
    is_l, is_r = owner == left, owner == right
    mask = jnp.concatenate([jnp.where(is_l, 1.0, 0.0), jnp.where(is_r, 1.0, 0.0)], axis=0).astype(BF16)
    n = fid.shape[0]
    upper = jnp.where(iota((128, 128), 0) < iota((128, 128), 1), 1.0, 0.0).astype(BF16)
    ri, ci = iota((2 * n, 2 * n), 0), iota((2 * n, 2 * n), 1)
    before = jnp.where((ci < ri) & ((ci < n) == (ri < n)), 1.0, 0.0).astype(BF16)
    ones = jnp.ones((128, 128), BF16)
    rank = dot(mask, upper) + dot(dot(before, mask).astype(BF16), ones)
    rank = rank.astype(I32)
    rank_l, rank_r = rank[:n], rank[n:]
    ext = jnp.where(is_l, store + rank_l, jnp.where(is_r, store + HALO + rank_r, off))
    return ext, off


def lanes_of(a):
    return jnp.concatenate([a[i:i + 1, :] for i in range(a.shape[0])], axis=1)


def ask_rows(ext, off, store):
    key = lanes_of(ext) - store
    offs = lanes_of(off)
    pick = jnp.where(iota((2 * HALO, key.shape[1]), 0) == key, 1.0, 0.0).astype(BF16)
    row = iota((16, key.shape[1]), 0)
    hi, lo = lax.shift_right_logical(offs, 6), lax.bitwise_and(offs, 63)
    parts = jnp.where(row == 0, hi, jnp.where(row == 1, lo, 0)).astype(F32).astype(BF16)
    got = dot(parts, pick, 1, 1).astype(I32)
    return got[0:1] * 64 + got[1:2]


def halo_kernel(group, fid_ref, x_ref, halo_ref, ext_ref, ask, ask_in, rep, rep_in, send, recv):
    me = lax.axis_index('g')
    left, right = lax.rem(me + group - 1, group), lax.rem(me + 1, group)
    barrier = pltpu.get_barrier_semaphore()
    for nb in (left, right):
        pl.semaphore_signal(barrier, inc=1, device_id=(nb,), device_id_type=MESH)
    feat, store = x_ref.shape
    half = rep.shape[1]
    ext, off = frontier_ext(fid_ref[...], me, group, store.bit_length() - 1)
    ext_ref[...] = ext
    ask[...] = jnp.broadcast_to(ask_rows(ext, off, store), ask.shape)
    pl.semaphore_wait(barrier, 2)
    asks = []
    for i, nb in enumerate((left, right)):
        asks.append(pltpu.make_async_remote_copy(ask, ask_in.at[i], send.at[i], recv.at[i], device_id=(nb,), device_id_type=MESH))
        asks[-1].start()
    for cp in asks:
        cp.wait_recv()
    lane = iota((1, 128), 1)
    want = jnp.where(lane < HALO, ask_in[0, 0:1, :], ask_in[1, 0:1, :])
    pick = jnp.where(iota((store, 128), 0) == want, 1.0, 0.0).astype(BF16)
    out = dot(x_ref[...], pick)
    pad = 2 * half - feat
    top = out[0:half]
    bot = jnp.concatenate([out[half:feat], jnp.zeros((pad, 128), F32)], axis=0)
    lo = iota((half, 128), 1) < HALO
    rep[0] = jnp.where(lo, top, pltpu.roll(bot, HALO, 1)).astype(BF16)
    rep[1] = jnp.where(lo, pltpu.roll(top, HALO, 1), bot).astype(BF16)
    reps = []
    for i, nb in enumerate((right, left)):
        reps.append(pltpu.make_async_remote_copy(rep.at[i], rep_in.at[i], send.at[2 + i], recv.at[2 + i], device_id=(nb,), device_id_type=MESH))
        reps[-1].start()
    for cp in reps:
        cp.wait_recv()
    from_l, from_r = rep_in[0].astype(F32), rep_in[1].astype(F32)
    halo_ref[0:half, :] = jnp.where(lo, from_l, pltpu.roll(from_r, HALO, 1)).astype(BF16)
    halo_ref[half:2 * half, :] = jnp.where(lo, pltpu.roll(from_l, HALO, 1), from_r).astype(BF16)
    for cp in asks + reps:
        cp.wait_send()


def local_kernel(scale, feat, classes, seeds, fan_one, fan_two,
                 x_ref, halo_ref, ext_ref, n1_ref, n2_ref, lab_ref, ws1_ref, wn1_ref, ws2_ref, wn2_ref,
                 g_ref, idx, acc, nf, z_ref):
    store = x_ref.shape[1]
    targets = n1_ref.shape[1]
    width = acc.shape[0]
    table = ext_ref[...]
    for r0 in range(0, n1_ref.shape[0], 8):
        for c0 in range(0, targets, 128):
            pos = n1_ref[r0:r0 + 8, c0:c0 + 128]
            hi = lax.shift_right_logical(pos, 7)
            lo = lax.bitwise_and(pos, 127)
            val = jnp.zeros((8, 128), I32)
            for h in range(table.shape[0]):
                row = jnp.broadcast_to(table[h:h + 1, :], (8, 128))
                val = jnp.where(hi == h, jnp.take_along_axis(row, lo, axis=1, mode='promise_in_bounds'), val)
            fld = jnp.zeros((8, 128), I32)
            for f in range(1, FIELDS):
                fld = fld + jnp.where(val >= f * width, 1, 0)
            idx[0, r0:r0 + 8, c0:c0 + 128] = val - fld * width
            idx[1, r0:r0 + 8, c0:c0 + 128] = lax.shift_left(jnp.ones((8, 128), I32), fld * FIELD_BITS)
    block = 16

    def count_block(b, carry):
        base = pl.multiple_of(b * block, block)
        for c0 in range(0, targets, 256):
            row = iota((block, 256), 0) + base
            tot = jnp.zeros((block, 256), I32)
            for k in range(fan_one):
                tot = tot + jnp.where(row == idx[0, k:k + 1, c0:c0 + 256], idx[1, k:k + 1, c0:c0 + 256], 0)
            acc[pl.ds(base, block), c0:c0 + 256] = tot
        return carry

    lax.fori_loop(0, width // block, count_block, 0)
    for f in range(FIELDS):
        part = lax.bitwise_and(lax.shift_right_logical(acc[...], f * FIELD_BITS), (1 << FIELD_BITS) - 1)
        nf[f * width:(f + 1) * width, targets:2 * targets] = part.astype(F32).astype(BF16)
    first = lanes_of(ext_ref[0:targets // 128, :])
    nf[:, 0:targets] = jnp.where(iota((nf.shape[0], targets), 0) == first, 1.0, 0.0).astype(BF16)

    halo = halo_ref[...]
    both = dot(x_ref[...], nf[0:store, :]) + dot(halo[0:feat], nf[store:store + 2 * HALO, :])
    x_t = both[:, 0:targets].astype(BF16)
    a_t = (both[:, targets:] * (1.0 / fan_one)).astype(BF16)
    z = dot(ws1_ref[...], x_t, 0, 0) + dot(wn1_ref[...], a_t, 0, 0)
    z_ref[...] = z
    h = jnp.maximum(z, 0.0).astype(BF16)
    lane = iota((1, 128), 1)
    m2 = jnp.zeros((targets, 128), F32)
    for k in range(fan_two):
        pos = jnp.where(lane < seeds, n2_ref[k:k + 1, :], -1)
        m2 = m2 + jnp.where(iota((targets, 128), 0) == pos, 1.0, 0.0)
    m2 = m2.astype(BF16)
    a2 = (dot(h, m2) * (1.0 / fan_two)).astype(BF16)
    hs = h[:, 0:128]
    cpad = ws2_ref.shape[0]
    crow = iota((cpad, 128), 0)
    wok = iota((cpad, 1), 0) < classes
    ws2 = jnp.where(wok, ws2_ref[...].astype(F32), 0.0).astype(BF16)
    wn2 = jnp.where(wok, wn2_ref[...].astype(F32), 0.0).astype(BF16)
    logits = dot(ws2, hs) + dot(wn2, a2)
    logits = jnp.where(crow < classes, logits, -1e30)
    top = jnp.max(logits, axis=0, keepdims=True)
    shifted = logits - top
    log_prob = shifted - jnp.log(jnp.sum(jnp.exp(shifted), axis=0, keepdims=True))
    label = jnp.where(lane < seeds, lab_ref[...], -1)
    hit = crow == label
    loss = -jnp.sum(jnp.where(hit, log_prob, 0.0))
    g = (jnp.exp(log_prob) - jnp.where(hit, 1.0, 0.0)) * scale
    g = jnp.where((crow < classes) & (lane < seeds), g, 0.0).astype(BF16)
    d_s2 = dot(g, hs, 1, 1)
    d_n2 = dot(g, a2, 1, 1)
    lrow = iota(d_s2.shape, 0) == classes
    d_s2 = jnp.where(lrow, loss, d_s2)
    g_seed = dot(ws2, g, 0, 0)
    g_agg = dot(wn2, g, 0, 0) * (1.0 / fan_two)
    p0 = g_agg.astype(BF16)
    r1 = g_agg - p0.astype(F32)
    p1 = r1.astype(BF16)
    p2 = (r1 - p1.astype(F32)).astype(BF16)
    d_h = dot(p0, m2, 1, 1) + (dot(p1, m2, 1, 1) + dot(p2, m2, 1, 1))
    d_h = d_h + jnp.concatenate([g_seed, jnp.zeros((g_seed.shape[0], targets - 128), F32)], axis=1)
    d_z = jnp.where(z_ref[...] > 0, d_h, 0.0).astype(BF16)
    tail = jnp.zeros((halo.shape[0] - feat, d_z.shape[0]), F32)
    at = 0
    for mat in (jnp.concatenate([dot(x_t, d_z, 1, 1), tail], axis=0),
                jnp.concatenate([dot(a_t, d_z, 1, 1), tail], axis=0), d_s2, d_n2):
        n = mat.shape[0] // 8
        for c0 in range(0, mat.shape[1], 128):
            g_ref[at:at + n] = mat[:, c0:c0 + 128].reshape(n, 8, 128)
            at += n
    g_ref[at:] = jnp.zeros((g_ref.shape[0] - at, 8, 128), F32)


def reduce_kernel(group, g_ref, r_ref, rc, part, l1a, l1b, w2a, w2b, l2a, l2b, zc, lz, zg, full, send, recv):
    nx, ny, nz = dims_of(group)
    ca, cb = CHUNK_A, CHUNK_B
    cx, cy, zn = ny * ca, nx * cb, ca + cb
    zsize = -(-zn // nz)
    off_b = nx * cx
    half = off_b + ny * cy
    me = lax.axis_index('g')
    core = lax.rem(me, 2)
    mx = lax.rem(me // 2, nx)
    my = lax.rem(me // (2 * nx), ny)
    mz = me // (2 * nx * ny)

    def dev(z, y, x, c):
        return ((z * ny + y) * nx + x) * 2 + c

    mate = dev(mz, my, mx, 1 - core)
    xs = [lax.rem(mx + d, nx) for d in range(nx)]
    ys = [lax.rem(my + d, ny) for d in range(ny)]
    zs = [lax.rem(mz + d, nz) for d in range(nz)]
    xdev = [dev(mz, my, x, core) for x in xs]
    ydev = [dev(mz, y, mx, core) for y in ys]
    zdev = [dev(z, my, mx, core) for z in zs]

    barrier = pltpu.get_barrier_semaphore()
    peers = [mate] + xdev[1:] + ydev[1:] + zdev[1:]
    for nb in peers:
        pl.semaphore_signal(barrier, inc=1, device_id=(nb,), device_id_type=MESH)
    pl.semaphore_wait(barrier, len(peers))

    copies = []

    def put(src, dst, to):
        k = len(copies)
        cp = pltpu.make_async_remote_copy(src, dst, send.at[k], recv.at[k], device_id=(to,), device_id_type=MESH)
        cp.start()
        copies.append(cp)
        return cp

    pieces = []
    for i in range(max(nx, ny)):
        if i < nx:
            d = (i + 1) % nx
            pieces.append((0, d, xs[d] * cx, cx))
        if i < ny:
            d = (i + 1) % ny
            pieces.append((1, d, off_b + ys[d] * cy, cy))
    other, mine = (1 - core) * half, core * half
    arrive = [put(g_ref.at[pl.ds(other + o, n)], rc.at[pl.ds(o, n)], mate) for _, _, o, n in pieces]
    in_a, in_b = [], []
    for (kind, d, o, n), cp in zip(pieces, arrive):
        cp.wait_recv()
        part[pl.ds(o, n)] = g_ref[pl.ds(mine + o, n)] + rc[pl.ds(o, n)]
        if d:
            if kind == 0:
                in_a.append((put(part.at[pl.ds(o, n)], l1a.at[d - 1], xdev[d]), d - 1))
            else:
                in_b.append((put(part.at[pl.ds(o, n)], l1b.at[d - 1], ydev[d]), d - 1))
    tot = part[pl.ds(mx * cx, cx)]
    for cp, s in in_a:
        cp.wait_recv()
        tot = tot + l1a[s]
    w2a[...] = tot
    in_a = [(put(w2a.at[pl.ds(ys[d] * ca, ca)], l2a.at[d - 1], ydev[d]), d - 1) for d in range(1, ny)]
    tot = part[pl.ds(off_b + my * cy, cy)]
    for cp, s in in_b:
        cp.wait_recv()
        tot = tot + l1b[s]
    w2b[...] = tot
    in_b = [(put(w2b.at[pl.ds(xs[d] * cb, cb)], l2b.at[d - 1], xdev[d]), d - 1) for d in range(1, nx)]
    tot = w2a[pl.ds(my * ca, ca)]
    for cp, s in in_a:
        cp.wait_recv()
        tot = tot + l2a[s]
    zc[0:ca] = tot
    tot = w2b[pl.ds(mx * cb, cb)]
    for cp, s in in_b:
        cp.wait_recv()
        tot = tot + l2b[s]
    zc[ca:zn] = tot
    in_z = [put(zc.at[pl.ds((zn * zs[d]) // nz, zsize)], lz.at[d - 1], zdev[d]) for d in range(1, nz)]
    tot = zc[pl.ds((zn * mz) // nz, zsize)]
    for s, cp in enumerate(in_z):
        cp.wait_recv()
        tot = tot + lz[s]
    zg[mz] = tot
    in_z = [put(zg.at[mz], zg.at[mz], zdev[d]) for d in range(1, nz)]
    for cp in in_z:
        cp.wait_recv()
    at_a = mine + mx * cx + my * ca
    at_b = mine + off_b + my * cy + mx * cb
    for z in range(nz):
        lo = (zn * z) // nz
        end = (zn * (z + 1)) // nz if z + 1 < nz else zn
        for t in range(lo, end):
            at = at_a + t if t < ca else at_b + (t - ca)
            full[pl.ds(at, 1)] = zg[z, t - lo:t - lo + 1]
    in_a = [put(full.at[pl.ds(at_a, ca)], full.at[pl.ds(at_a, ca)], ydev[d]) for d in range(1, ny)]
    in_b = [put(full.at[pl.ds(at_b, cb)], full.at[pl.ds(at_b, cb)], xdev[d]) for d in range(1, nx)]
    row_a, row_b = mine + mx * cx, mine + off_b + my * cy
    for cp in in_a:
        cp.wait_recv()
    in_a = [put(full.at[pl.ds(row_a, cx)], full.at[pl.ds(row_a, cx)], xdev[d]) for d in range(1, nx)]
    for cp in in_b:
        cp.wait_recv()
    in_b = [put(full.at[pl.ds(row_b, cy)], full.at[pl.ds(row_b, cy)], ydev[d]) for d in range(1, ny)]
    back = [put(full.at[pl.ds(row_a, cx)], full.at[pl.ds(row_a, cx)], mate),
            put(full.at[pl.ds(row_b, cy)], full.at[pl.ds(row_b, cy)], mate)]
    for i in range(max(nx, ny) - 1):
        if i < nx - 1:
            in_a[i].wait_recv()
            at = mine + lax.rem(mx + nx - 1 - i, nx) * cx
            back.append(put(full.at[pl.ds(at, cx)], full.at[pl.ds(at, cx)], mate))
        if i < ny - 1:
            in_b[i].wait_recv()
            at = mine + off_b + lax.rem(my + ny - 1 - i, ny) * cy
            back.append(put(full.at[pl.ds(at, cy)], full.at[pl.ds(at, cy)], mate))
    for cp in back:
        cp.wait_recv()
    for cp in copies:
        cp.wait_send()
    r_ref[...] = full[...]


def copy_count(group):
    nx, ny, nz = dims_of(group)
    return 2 * (nx + ny) + 4 * (nx - 1 + ny - 1) + 2 * (nz - 1)


def reduce_call(group, tiles):
    nx, ny, nz = dims_of(group)
    ca, cb = CHUNK_A, CHUNK_B
    cx, cy, zn = ny * ca, nx * cb, ca + cb
    zsize = -(-zn // nz)
    half = nx * cx + ny * cy
    total = 2 * half
    n = copy_count(group)

    def buf(*lead):
        return VMEM((*lead, 8, 128), F32)

    return pl.pallas_call(
        functools.partial(reduce_kernel, group),
        name='gradient_sum',
        out_shape=jax.ShapeDtypeStruct((total, 8, 128), F32),
        in_specs=[pl.BlockSpec(memory_space=VMEM)],
        out_specs=pl.BlockSpec(memory_space=VMEM),
        scratch_shapes=[buf(half), buf(half), buf(nx - 1, cx), buf(ny - 1, cy), buf(cx), buf(cy),
                        buf(ny - 1, ca), buf(nx - 1, cb), buf(zn), buf(nz - 1, zsize), buf(nz, zsize), buf(total),
                        pltpu.SemaphoreType.DMA((n,)), pltpu.SemaphoreType.DMA((n,))],
        compiler_params=pltpu.CompilerParams(collective_id=1, has_side_effects=True),
    )(tiles)


def output_kernel(scale, r_ref, loss_ref, s1_ref, n1_ref, s2_ref, n2_ref):
    at = 0
    classes = s2_ref.shape[0]
    for ref in (s1_ref, n1_ref, s2_ref, n2_ref):
        rows, cols = ref.shape
        n = -(-rows // 8)
        for c0 in range(0, cols, 128):
            val = r_ref[at:at + n].reshape(n * 8, 128)
            ref[:, c0:c0 + 128] = val[0:rows]
            if ref is s2_ref and c0 == 0:
                loss_ref[...] = val[classes:classes + 1, 0:1] * scale
            at += n


def solution(mesh):
    group = mesh.shape['g']

    def device_step(x_local, front_ids, nbr_one, nbr_two, labels, w_self1, w_nbr1, w_self2, w_nbr2):
        store, feat = x_local.shape
        targets, fan_one = nbr_one.shape
        seeds, fan_two = nbr_two.shape
        hidden, classes = w_self2.shape
        frows = -(-feat // 32) * 32
        scale = 1.0 / (group * seeds)
        x_t = x_local.T
        fid = front_ids.reshape(-1, 128)
        vm = pl.BlockSpec(memory_space=VMEM)
        halo, ext = pl.pallas_call(
            functools.partial(halo_kernel, group),
            name='halo_rows',
            out_shape=[jax.ShapeDtypeStruct((frows, 2 * HALO), BF16), jax.ShapeDtypeStruct(fid.shape, I32)],
            in_specs=[vm, vm], out_specs=[vm, vm],
            scratch_shapes=[VMEM((8, 128), I32), VMEM((2, 8, 128), I32), VMEM((2, frows // 2, 128), BF16),
                            VMEM((2, frows // 2, 128), BF16), pltpu.SemaphoreType.DMA((4,)), pltpu.SemaphoreType.DMA((4,))],
            compiler_params=pltpu.CompilerParams(collective_id=0, has_side_effects=True),
        )(fid, x_t)
        width = -(-(store + 2 * HALO) // (FIELDS * 16)) * 16
        nx, ny, nz = dims_of(group)
        tiles = 2 * nx * ny * (CHUNK_A + CHUNK_B)
        tiles = max(tiles, 352)
        kpad, cpad = -(-fan_one // 8) * 8, -(-classes // 16) * 16

        def full(*shape):
            return pl.BlockSpec(shape, lambda i: (0,) * len(shape))

        grads = pl.pallas_call(
            functools.partial(local_kernel, scale, feat, classes, seeds, fan_one, fan_two),
            name='local_step',
            grid=(1,),
            out_shape=jax.ShapeDtypeStruct((tiles, 8, 128), F32),
            in_specs=[full(feat, store), full(frows, 2 * HALO), full(*fid.shape), full(kpad, targets), full(16, 128),
                      full(1, 128), full(feat, hidden), full(feat, hidden), full(cpad, hidden), full(cpad, hidden)],
            out_specs=full(tiles, 8, 128),
            scratch_shapes=[VMEM((2, kpad, targets), I32), VMEM((width, targets), I32),
                            VMEM((FIELDS * width, 2 * targets), BF16), VMEM((hidden, targets), F32)],
            compiler_params=pltpu.CompilerParams(vmem_limit_bytes=60 * 1024 * 1024),
        )(x_t, halo, ext, nbr_one.T, nbr_two.T, labels.reshape(1, -1), w_self1, w_nbr1, w_self2.T, w_nbr2.T)
        if group == 256:
            sums = reduce_call(group, grads)
        else:
            step = 2 * nx * ny * (CHUNK_A + CHUNK_B)
            sums = jnp.concatenate([reduce_call(group, grads[i:i + step]) for i in range(0, tiles, step)])
        loss, d_s1, d_n1, d_s2, d_n2 = pl.pallas_call(
            functools.partial(output_kernel, scale),
            name='split_outputs',
            out_shape=[jax.ShapeDtypeStruct((1, 1), F32), jax.ShapeDtypeStruct((feat, hidden), F32),
                       jax.ShapeDtypeStruct((feat, hidden), F32), jax.ShapeDtypeStruct((classes, hidden), F32),
                       jax.ShapeDtypeStruct((classes, hidden), F32)],
            in_specs=[vm], out_specs=[vm] * 5,
        )(sums)
        return loss[0, 0], d_s1, d_n1, d_s2.T, d_n2.T

    return jax.shard_map(device_step, mesh=mesh,
                         in_specs=(P('g', None), P('g'), P('g', None), P('g', None), P('g'), P(), P(), P(), P()),
                         out_specs=(P(), P(), P(), P(), P()), check_vma=False)
```

```python
import functools

import jax
import jax.numpy as jnp
from jax import lax
from jax.experimental import pallas as pl
from jax.experimental.pallas import tpu as pltpu
from jax.sharding import PartitionSpec as P

MESH = pl.DeviceIdType.MESH
F32, BF16, I32 = jnp.float32, jnp.bfloat16, jnp.int32
VMEM = pltpu.VMEM

HALO = 64
FIELDS, FIELD_BITS = 6, 5


def dims_of(group):
    return {256: (4, 4, 8), 16: (2, 2, 2)}[group]


def chunks_of(group):
    return {256: (6, 5), 16: (21, 20)}[group]


def dot(a, b, ca=1, cb=0):
    return lax.dot_general(a, b, (((ca,), (cb,)), ((), ())), preferred_element_type=F32)


def iota(shape, dim):
    return lax.broadcasted_iota(I32, shape, dim)


def frontier_ext(fid, me, group, rows_log2):
    store = 1 << rows_log2
    owner = lax.shift_right_logical(fid, rows_log2)
    off = lax.bitwise_and(fid, store - 1)
    left, right = lax.rem(me + group - 1, group), lax.rem(me + 1, group)
    is_l, is_r = owner == left, owner == right
    mask = jnp.concatenate([jnp.where(is_l, 1.0, 0.0), jnp.where(is_r, 1.0, 0.0)], axis=0).astype(BF16)
    n = fid.shape[0]
    upper = jnp.where(iota((128, 128), 0) < iota((128, 128), 1), 1.0, 0.0).astype(BF16)
    ri, ci = iota((2 * n, 2 * n), 0), iota((2 * n, 2 * n), 1)
    before = jnp.where((ci < ri) & ((ci < n) == (ri < n)), 1.0, 0.0).astype(BF16)
    ones = jnp.ones((128, 128), BF16)
    rank = dot(mask, upper) + dot(dot(before, mask).astype(BF16), ones)
    rank = rank.astype(I32)
    rank_l, rank_r = rank[:n], rank[n:]
    ext = jnp.where(is_l, store + rank_l, jnp.where(is_r, store + HALO + rank_r, off))
    return ext, off


def lanes_of(a):
    return jnp.concatenate([a[i:i + 1, :] for i in range(a.shape[0])], axis=1)


def ask_rows(ext, off, store):
    key = lanes_of(ext) - store
    offs = lanes_of(off)
    pick = jnp.where(iota((2 * HALO, key.shape[1]), 0) == key, 1.0, 0.0).astype(BF16)
    row = iota((16, key.shape[1]), 0)
    hi, lo = lax.shift_right_logical(offs, 6), lax.bitwise_and(offs, 63)
    parts = jnp.where(row == 0, hi, jnp.where(row == 1, lo, 0)).astype(F32).astype(BF16)
    got = dot(parts, pick, 1, 1).astype(I32)
    return got[0:1] * 64 + got[1:2]


def step_kernel(group, scale, fid_ref, x_hbm, n1_ref, n2_ref, lab_ref, ws1_hbm, wn1_hbm, ws2_ref, wn2_ref, r_ref,
                x_ref, ws1_ref, wn1_ref, in_sem, ask, ask_in, rep, rep_in, hsend, hrecv,
                small, idx, acc, nf, both, z_ref, gpad, g,
                rc, part, l1a, l1b, w2a, w2b, l2a, l2b, zc, lz, zg, full, send, recv):
    nx, ny, nz = dims_of(group)
    ca, cb = chunks_of(group)
    cx, cy, zn = ny * ca, nx * cb, ca + cb
    zsize = -(-zn // nz)
    off_b = nx * cx
    half = off_b + ny * cy
    me = lax.axis_index('g')
    core = lax.rem(me, 2)
    mx = lax.rem(me // 2, nx)
    my = lax.rem(me // (2 * nx), ny)
    mz = me // (2 * nx * ny)

    def dev(z, y, x, c):
        return ((z * ny + y) * nx + x) * 2 + c

    mate = dev(mz, my, mx, 1 - core)
    xs = [lax.rem(mx + d, nx) for d in range(nx)]
    ys = [lax.rem(my + d, ny) for d in range(ny)]
    zs = [lax.rem(mz + d, nz) for d in range(nz)]
    xdev = [dev(mz, my, x, core) for x in xs]
    ydev = [dev(mz, y, mx, core) for y in ys]
    zdev = [dev(z, my, mx, core) for z in zs]
    left, right = lax.rem(me + group - 1, group), lax.rem(me + 1, group)

    barrier = pltpu.get_barrier_semaphore()
    peers = [left, right, mate] + xdev[1:] + ydev[1:] + zdev[1:]
    for nb in peers:
        pl.semaphore_signal(barrier, inc=1, device_id=(nb,), device_id_type=MESH)
    loads = [pltpu.make_async_copy(s, d, in_sem.at[i]) for i, (s, d) in
             enumerate(((x_hbm, x_ref), (ws1_hbm, ws1_ref), (wn1_hbm, wn1_ref)))]
    for cp in loads:
        cp.start()

    feat, store = x_ref.shape
    targets = n1_ref.shape[1]
    fan_one = n1_ref.shape[0]
    fan_two, seeds = n2_ref.shape
    classes = ws2_ref.shape[0]
    width = acc.shape[0]
    hrows = rep.shape[1]
    ext, off = frontier_ext(fid_ref[...], me, group, store.bit_length() - 1)
    ask[...] = jnp.broadcast_to(ask_rows(ext, off, store), ask.shape)
    pl.semaphore_wait(barrier, len(peers))
    asks = []
    for i, nb in enumerate((left, right)):
        asks.append(pltpu.make_async_remote_copy(ask, ask_in.at[i], hsend.at[i], hrecv.at[i], device_id=(nb,), device_id_type=MESH))
        asks[-1].start()

    for r0 in range(0, fan_one, 8):
        nr = min(8, fan_one - r0)
        for c0 in range(0, targets, 128):
            pos = n1_ref[r0:r0 + nr, c0:c0 + 128]
            if nr < 8:
                pos = jnp.broadcast_to(pos[0:1], (8, 128)) if nr == 1 else jnp.concatenate([pos, pos[0:8 - nr]], axis=0)
            hi = lax.shift_right_logical(pos, 7)
            lo = lax.bitwise_and(pos, 127)
            val = jnp.zeros((8, 128), I32)
            for h in range(ext.shape[0]):
                row = jnp.broadcast_to(ext[h:h + 1, :], (8, 128))
                val = jnp.where(hi == h, jnp.take_along_axis(row, lo, axis=1, mode='promise_in_bounds'), val)
            fld = jnp.zeros((8, 128), I32)
            for f in range(1, FIELDS):
                fld = fld + jnp.where(val >= f * width, 1, 0)
            idx[0, r0:r0 + 8, c0:c0 + 128] = val - fld * width
            idx[1, r0:r0 + 8, c0:c0 + 128] = lax.shift_left(jnp.ones((8, 128), I32), fld * FIELD_BITS)
    first = lanes_of(ext[0:targets // 128, :])
    nf[:, 0:targets] = jnp.where(iota((nf.shape[0], targets), 0) == first, 1.0, 0.0).astype(BF16)

    for cp in asks:
        cp.wait_recv()
    lane = iota((1, 128), 1)
    want = jnp.where(lane < HALO, ask_in[0, 0:1, :], ask_in[1, 0:1, :])
    pick = jnp.where(iota((store, 128), 0) == want, 1.0, 0.0).astype(BF16)
    loads[0].wait()
    out = dot(x_ref[...], pick)
    top = out[0:hrows]
    bot = jnp.concatenate([out[hrows:feat], jnp.zeros((2 * hrows - feat, 128), F32)], axis=0)
    low = iota((hrows, 128), 1) < HALO
    rep[0] = jnp.where(low, top, pltpu.roll(bot, HALO, 1)).astype(BF16)
    rep[1] = jnp.where(low, pltpu.roll(top, HALO, 1), bot).astype(BF16)
    reps = []
    for i, nb in enumerate((right, left)):
        reps.append(pltpu.make_async_remote_copy(rep.at[i], rep_in.at[i], hsend.at[2 + i], hrecv.at[2 + i], device_id=(nb,), device_id_type=MESH))
        reps[-1].start()

    block = 16

    def count_block(b, carry):
        base = pl.multiple_of(b * block, block)
        for c0 in range(0, targets, 256):
            row = iota((block, 256), 0) + base
            tot = jnp.zeros((block, 256), I32)
            for k in range(fan_one):
                tot = tot + jnp.where(row == idx[0, k:k + 1, c0:c0 + 256], idx[1, k:k + 1, c0:c0 + 256], 0)
            acc[pl.ds(base, block), c0:c0 + 256] = tot
        return carry

    lax.fori_loop(0, width // block, count_block, 0)
    for f in range(FIELDS):
        cnt = lax.bitwise_and(lax.shift_right_logical(acc[...], f * FIELD_BITS), (1 << FIELD_BITS) - 1)
        nf[f * width:(f + 1) * width, targets:2 * targets] = cnt.astype(F32).astype(BF16)
    both[...] = dot(x_ref[...], nf[0:store, :])

    small[...] = jnp.full(small.shape, -1, I32)
    small[0:fan_two, 0:seeds] = n2_ref[...]
    small[12:13, 0:seeds] = lab_ref[...]
    m2 = jnp.zeros((targets, 128), F32)
    for k in range(fan_two):
        m2 = m2 + jnp.where(iota((targets, 128), 0) == small[k:k + 1, :], 1.0, 0.0)
    m2 = m2.astype(BF16)

    for cp in reps:
        cp.wait_recv()
    from_l, from_r = rep_in[0].astype(F32), rep_in[1].astype(F32)
    halo = jnp.concatenate([jnp.where(low, from_l, pltpu.roll(from_r, HALO, 1)).astype(BF16),
                            jnp.where(low, pltpu.roll(from_l, HALO, 1), from_r).astype(BF16)], axis=0)
    rows = both[...] + dot(halo[0:feat], nf[store:store + 2 * HALO, :])
    x_t = rows[:, 0:targets].astype(BF16)
    a_t = (rows[:, targets:] * (1.0 / fan_one)).astype(BF16)
    loads[1].wait()
    loads[2].wait()
    z = dot(ws1_ref[...], x_t, 0, 0) + dot(wn1_ref[...], a_t, 0, 0)
    z_ref[...] = z
    h = jnp.maximum(z, 0.0).astype(BF16)
    a2 = (dot(h, m2) * (1.0 / fan_two)).astype(BF16)
    hs = h[:, 0:128]
    ws2, wn2 = ws2_ref[...], wn2_ref[...]
    logits = dot(ws2, hs) + dot(wn2, a2)
    shifted = logits - jnp.max(logits, axis=0, keepdims=True)
    log_prob = shifted - jnp.log(jnp.sum(jnp.exp(shifted), axis=0, keepdims=True))
    hit = iota(logits.shape, 0) == small[12:13, :]
    loss = -jnp.sum(jnp.where(hit, log_prob, 0.0))
    gl = (jnp.exp(log_prob) - jnp.where(hit, 1.0, 0.0)) * scale
    gpad[...] = jnp.zeros(gpad.shape, F32)
    gpad[0:classes, :] = jnp.where(lane < seeds, gl, 0.0)
    gb = gpad[...].astype(BF16)
    d_s2 = dot(gb, hs, 1, 1)
    d_n2 = dot(gb, a2, 1, 1)
    d_s2 = jnp.where(iota(d_s2.shape, 0) == classes, loss, d_s2)
    gc = gb[0:classes]
    g_seed = dot(ws2, gc, 0, 0)
    g_agg = dot(wn2, gc, 0, 0) * (1.0 / fan_two)
    p0 = g_agg.astype(BF16)
    r1 = g_agg - p0.astype(F32)
    p1 = r1.astype(BF16)
    p2 = (r1 - p1.astype(F32)).astype(BF16)
    d_h = dot(p0, m2, 1, 1) + (dot(p1, m2, 1, 1) + dot(p2, m2, 1, 1))
    d_h = d_h + jnp.concatenate([g_seed, jnp.zeros((g_seed.shape[0], targets - 128), F32)], axis=1)
    d_z = jnp.where(z_ref[...] > 0, d_h, 0.0).astype(BF16)
    tail = jnp.zeros((2 * hrows - feat, d_z.shape[0]), F32)
    at = 0
    for mat in (jnp.concatenate([dot(x_t, d_z, 1, 1), tail], axis=0),
                jnp.concatenate([dot(a_t, d_z, 1, 1), tail], axis=0), d_s2, d_n2):
        n = mat.shape[0] // 8
        for c0 in range(0, mat.shape[1], 128):
            g[at:at + n] = mat[:, c0:c0 + 128].reshape(n, 8, 128)
            at += n
    g[at:] = jnp.zeros((g.shape[0] - at, 8, 128), F32)

    copies = []

    def put(src, dst, to):
        k = len(copies)
        cp = pltpu.make_async_remote_copy(src, dst, send.at[k], recv.at[k], device_id=(to,), device_id_type=MESH)
        cp.start()
        copies.append(cp)
        return cp

    pieces = []
    for i in range(max(nx, ny)):
        if i < nx:
            d = (i + 1) % nx
            pieces.append((0, d, xs[d] * cx, cx))
        if i < ny:
            d = (i + 1) % ny
            pieces.append((1, d, off_b + ys[d] * cy, cy))
    other, mine = (1 - core) * half, core * half
    arrive = [put(g.at[pl.ds(other + o, n)], rc.at[pl.ds(o, n)], mate) for _, _, o, n in pieces]
    in_a, in_b = [], []
    for (kind, d, o, n), cp in zip(pieces, arrive):
        cp.wait_recv()
        part[pl.ds(o, n)] = g[pl.ds(mine + o, n)] + rc[pl.ds(o, n)]
        if d:
            if kind == 0:
                in_a.append((put(part.at[pl.ds(o, n)], l1a.at[d - 1], xdev[d]), d - 1))
            else:
                in_b.append((put(part.at[pl.ds(o, n)], l1b.at[d - 1], ydev[d]), d - 1))
    tot = part[pl.ds(mx * cx, cx)]
    for cp, s in in_a:
        cp.wait_recv()
        tot = tot + l1a[s]
    w2a[...] = tot
    in_a = [(put(w2a.at[pl.ds(ys[d] * ca, ca)], l2a.at[d - 1], ydev[d]), d - 1) for d in range(1, ny)]
    tot = part[pl.ds(off_b + my * cy, cy)]
    for cp, s in in_b:
        cp.wait_recv()
        tot = tot + l1b[s]
    w2b[...] = tot
    in_b = [(put(w2b.at[pl.ds(xs[d] * cb, cb)], l2b.at[d - 1], xdev[d]), d - 1) for d in range(1, nx)]
    tot = w2a[pl.ds(my * ca, ca)]
    for cp, s in in_a:
        cp.wait_recv()
        tot = tot + l2a[s]
    zc[0:ca] = tot
    tot = w2b[pl.ds(mx * cb, cb)]
    for cp, s in in_b:
        cp.wait_recv()
        tot = tot + l2b[s]
    zc[ca:zn] = tot
    in_z = [put(zc.at[pl.ds((zn * zs[d]) // nz, zsize)], lz.at[d - 1], zdev[d]) for d in range(1, nz)]
    tot = zc[pl.ds((zn * mz) // nz, zsize)]
    for s, cp in enumerate(in_z):
        cp.wait_recv()
        tot = tot + lz[s]
    zg[mz] = tot
    in_z = [put(zg.at[mz], zg.at[mz], zdev[d]) for d in range(1, nz)]
    for cp in in_z:
        cp.wait_recv()
    at_a = mine + mx * cx + my * ca
    at_b = mine + off_b + my * cy + mx * cb
    for z in range(nz):
        lo = (zn * z) // nz
        end = (zn * (z + 1)) // nz if z + 1 < nz else zn
        for t in range(lo, end):
            at = at_a + t if t < ca else at_b + (t - ca)
            full[pl.ds(at, 1)] = zg[z, t - lo:t - lo + 1]
    in_a = [put(full.at[pl.ds(at_a, ca)], full.at[pl.ds(at_a, ca)], ydev[d]) for d in range(1, ny)]
    in_b = [put(full.at[pl.ds(at_b, cb)], full.at[pl.ds(at_b, cb)], xdev[d]) for d in range(1, nx)]
    row_a, row_b = mine + mx * cx, mine + off_b + my * cy
    for cp in in_a:
        cp.wait_recv()
    in_a = [put(full.at[pl.ds(row_a, cx)], full.at[pl.ds(row_a, cx)], xdev[d]) for d in range(1, nx)]
    for cp in in_b:
        cp.wait_recv()
    in_b = [put(full.at[pl.ds(row_b, cy)], full.at[pl.ds(row_b, cy)], ydev[d]) for d in range(1, ny)]
    back = [put(full.at[pl.ds(row_a, cx)], full.at[pl.ds(row_a, cx)], mate),
            put(full.at[pl.ds(row_b, cy)], full.at[pl.ds(row_b, cy)], mate)]
    for i in range(max(nx, ny) - 1):
        if i < nx - 1:
            in_a[i].wait_recv()
            at = mine + lax.rem(mx + nx - 1 - i, nx) * cx
            back.append(put(full.at[pl.ds(at, cx)], full.at[pl.ds(at, cx)], mate))
        if i < ny - 1:
            in_b[i].wait_recv()
            at = mine + off_b + lax.rem(my + ny - 1 - i, ny) * cy
            back.append(put(full.at[pl.ds(at, cy)], full.at[pl.ds(at, cy)], mate))
    for cp in back:
        cp.wait_recv()
    for cp in copies:
        cp.wait_send()
    for cp in asks + reps:
        cp.wait_send()
    r_ref[...] = full[...]


def copy_count(group):
    nx, ny, nz = dims_of(group)
    return 2 * (nx + ny) + 4 * (nx - 1 + ny - 1) + 2 * (nz - 1)


def output_kernel(scale, r_ref, loss_ref, s1_ref, n1_ref, s2_ref, n2_ref):
    at = 0
    classes = s2_ref.shape[0]
    for ref in (s1_ref, n1_ref, s2_ref, n2_ref):
        rows, cols = ref.shape
        n = -(-rows // 8)
        for c0 in range(0, cols, 128):
            val = r_ref[at:at + n].reshape(n * 8, 128)
            ref[:, c0:c0 + 128] = val[0:rows]
            if ref is s2_ref and c0 == 0:
                loss_ref[...] = val[classes:classes + 1, 0:1] * scale
            at += n


def solution(mesh):
    group = mesh.shape['g']

    def device_step(x_local, front_ids, nbr_one, nbr_two, labels, w_self1, w_nbr1, w_self2, w_nbr2):
        store, feat = x_local.shape
        targets, fan_one = nbr_one.shape
        seeds = nbr_two.shape[0]
        hidden, classes = w_self2.shape
        frows = -(-feat // 32) * 32
        scale = 1.0 / (group * seeds)
        fid = front_ids.reshape(-1, 128)
        width = -(-(store + 2 * HALO) // (FIELDS * 16)) * 16
        nx, ny, nz = dims_of(group)
        ca, cb = chunks_of(group)
        cx, cy, zn = ny * ca, nx * cb, ca + cb
        zsize = -(-zn // nz)
        half = nx * cx + ny * cy
        total = 2 * half
        n = copy_count(group)
        dma = pltpu.SemaphoreType.DMA

        def buf(*lead):
            return VMEM((*lead, 8, 128), F32)

        vm, hbm = pl.BlockSpec(memory_space=VMEM), pl.BlockSpec(memory_space=pl.ANY)
        sums = pl.pallas_call(
            functools.partial(step_kernel, group, scale),
            name='train_step',
            out_shape=jax.ShapeDtypeStruct((total, 8, 128), F32),
            in_specs=[vm, hbm, vm, vm, vm, hbm, hbm, vm, vm],
            out_specs=vm,
            scratch_shapes=[
                VMEM((feat, store), BF16), VMEM((feat, hidden), BF16), VMEM((feat, hidden), BF16), dma((3,)),
                VMEM((8, 128), I32), VMEM((2, 8, 128), I32), VMEM((2, frows // 2, 128), BF16),
                VMEM((2, frows // 2, 128), BF16), dma((4,)), dma((4,)),
                VMEM((16, 128), I32), VMEM((2, -(-fan_one // 8) * 8, targets), I32), VMEM((width, targets), I32),
                VMEM((FIELDS * width, 2 * targets), BF16), VMEM((feat, 2 * targets), F32), VMEM((hidden, targets), F32),
                VMEM((-(-classes // 16) * 16, 128), F32), buf(total),
                buf(half), buf(half), buf(nx - 1, cx), buf(ny - 1, cy), buf(cx), buf(cy),
                buf(ny - 1, ca), buf(nx - 1, cb), buf(zn), buf(nz - 1, zsize), buf(nz, zsize), buf(total),
                dma((n,)), dma((n,))],
            compiler_params=pltpu.CompilerParams(collective_id=0, has_side_effects=True,
                                                 vmem_limit_bytes=60 * 1024 * 1024),
        )(fid, x_local.T, nbr_one.T, nbr_two.T, labels.reshape(1, -1), w_self1, w_nbr1, w_self2.T, w_nbr2.T)
        loss, d_s1, d_n1, d_s2, d_n2 = pl.pallas_call(
            functools.partial(output_kernel, scale),
            name='split_outputs',
            out_shape=[jax.ShapeDtypeStruct((1, 1), F32), jax.ShapeDtypeStruct((feat, hidden), F32),
                       jax.ShapeDtypeStruct((feat, hidden), F32), jax.ShapeDtypeStruct((classes, hidden), F32),
                       jax.ShapeDtypeStruct((classes, hidden), F32)],
            in_specs=[vm], out_specs=[vm] * 5,
        )(sums)
        return loss[0, 0], d_s1, d_n1, d_s2.T, d_n2.T

    return jax.shard_map(device_step, mesh=mesh,
                         in_specs=(P('g', None), P('g'), P('g', None), P('g', None), P('g'), P(), P(), P(), P()),
                         out_specs=(P(), P(), P(), P(), P()), check_vma=False)
```

```python
import functools

import jax
import jax.numpy as jnp
from jax import lax
from jax.experimental import pallas as pl
from jax.experimental.pallas import tpu as pltpu
from jax.sharding import PartitionSpec as P

MESH = pl.DeviceIdType.MESH
F32, BF16, I32 = jnp.float32, jnp.bfloat16, jnp.int32
VMEM = pltpu.VMEM

HALO = 64
FIELDS, FIELD_BITS = 6, 5


def dims_of(group):
    return {256: (4, 4, 8), 16: (2, 2, 2)}[group]


def chunks_of(group):
    return {256: (6, 5), 16: (21, 20)}[group]


def dot(a, b, ca=1, cb=0):
    return lax.dot_general(a, b, (((ca,), (cb,)), ((), ())), preferred_element_type=F32)


def iota(shape, dim):
    return lax.broadcasted_iota(I32, shape, dim)


def frontier_ext(fid, me, group, rows_log2):
    store = 1 << rows_log2
    owner = lax.shift_right_logical(fid, rows_log2)
    off = lax.bitwise_and(fid, store - 1)
    left, right = lax.rem(me + group - 1, group), lax.rem(me + 1, group)
    is_l, is_r = owner == left, owner == right
    mask = jnp.concatenate([jnp.where(is_l, 1.0, 0.0), jnp.where(is_r, 1.0, 0.0)], axis=0).astype(BF16)
    n = fid.shape[0]
    upper = jnp.where(iota((128, 128), 0) < iota((128, 128), 1), 1.0, 0.0).astype(BF16)
    ri, ci = iota((2 * n, 2 * n), 0), iota((2 * n, 2 * n), 1)
    before = jnp.where((ci < ri) & ((ci < n) == (ri < n)), 1.0, 0.0).astype(BF16)
    ones = jnp.ones((128, 128), BF16)
    rank = dot(mask, upper) + dot(dot(before, mask).astype(BF16), ones)
    rank = rank.astype(I32)
    rank_l, rank_r = rank[:n], rank[n:]
    ext = jnp.where(is_l, store + rank_l, jnp.where(is_r, store + HALO + rank_r, off))
    return ext, off


def lanes_of(a):
    return jnp.concatenate([a[i:i + 1, :] for i in range(a.shape[0])], axis=1)


def ask_rows(ext, off, store):
    key = lanes_of(ext) - store
    offs = lanes_of(off)
    pick = jnp.where(iota((2 * HALO, key.shape[1]), 0) == key, 1.0, 0.0).astype(BF16)
    row = iota((16, key.shape[1]), 0)
    hi, lo = lax.shift_right_logical(offs, 6), lax.bitwise_and(offs, 63)
    parts = jnp.where(row == 0, hi, jnp.where(row == 1, lo, 0)).astype(F32).astype(BF16)
    got = dot(parts, pick, 1, 1).astype(I32)
    return got[0:1] * 64 + got[1:2]


def step_kernel(group, scale, fid_ref, x_hbm, n1_ref, n2_ref, lab_ref, ws1_hbm, wn1_hbm, ws2_ref, wn2_ref, r_ref,
                x_ref, ws1_ref, wn1_ref, in_sem, ask, ask_in, rep, rep_in, hsend, hrecv,
                small, idx, acc, nf, both, z_ref, gpad, g,
                rc, part, l1a, l1b, w2a, w2b, l2a, l2b, zc, lz, zg, full, send, recv):
    nx, ny, nz = dims_of(group)
    ca, cb = chunks_of(group)
    cx, cy, zn = ny * ca, nx * cb, ca + cb
    nq = max(1, nz // 2)
    zsize = -(-zn // nq)
    off_b = nx * cx
    half = off_b + ny * cy
    me = lax.axis_index('g')
    core = lax.rem(me, 2)
    mx = lax.rem(me // 2, nx)
    my = lax.rem(me // (2 * nx), ny)
    mz = me // (2 * nx * ny)

    def dev(z, y, x, c):
        return ((z * ny + y) * nx + x) * 2 + c

    mate = dev(mz, my, mx, 1 - core)
    xs = [lax.rem(mx + d, nx) for d in range(nx)]
    ys = [lax.rem(my + d, ny) for d in range(ny)]
    zs = [lax.rem(mz + d, nz) for d in range(nz)]
    xdev = [dev(mz, my, x, core) for x in xs]
    ydev = [dev(mz, y, mx, core) for y in ys]
    zdev = [dev(z, my, mx, core) for z in zs]
    left, right = lax.rem(me + group - 1, group), lax.rem(me + 1, group)

    barrier = pltpu.get_barrier_semaphore()
    peers = [left, right, mate] + xdev[1:] + ydev[1:] + zdev[1:]
    for nb in peers:
        pl.semaphore_signal(barrier, inc=1, device_id=(nb,), device_id_type=MESH)
    loads = [pltpu.make_async_copy(s, d, in_sem.at[i]) for i, (s, d) in
             enumerate(((x_hbm, x_ref), (ws1_hbm, ws1_ref), (wn1_hbm, wn1_ref)))]
    for cp in loads:
        cp.start()

    feat, store = x_ref.shape
    targets = n1_ref.shape[1]
    fan_one = n1_ref.shape[0]
    fan_two, seeds = n2_ref.shape
    classes = ws2_ref.shape[0]
    width = acc.shape[0]
    hrows = rep.shape[1]
    ext, off = frontier_ext(fid_ref[...], me, group, store.bit_length() - 1)
    ask[...] = jnp.broadcast_to(ask_rows(ext, off, store), ask.shape)
    pl.semaphore_wait(barrier, len(peers))
    asks = []
    for i, nb in enumerate((left, right)):
        asks.append(pltpu.make_async_remote_copy(ask, ask_in.at[i], hsend.at[i], hrecv.at[i], device_id=(nb,), device_id_type=MESH))
        asks[-1].start()

    for r0 in range(0, fan_one, 8):
        nr = min(8, fan_one - r0)
        for c0 in range(0, targets, 128):
            pos = n1_ref[r0:r0 + nr, c0:c0 + 128]
            if nr < 8:
                pos = jnp.broadcast_to(pos[0:1], (8, 128)) if nr == 1 else jnp.concatenate([pos, pos[0:8 - nr]], axis=0)
            hi = lax.shift_right_logical(pos, 7)
            lo = lax.bitwise_and(pos, 127)
            val = jnp.zeros((8, 128), I32)
            for h in range(ext.shape[0]):
                row = jnp.broadcast_to(ext[h:h + 1, :], (8, 128))
                val = jnp.where(hi == h, jnp.take_along_axis(row, lo, axis=1, mode='promise_in_bounds'), val)
            fld = jnp.zeros((8, 128), I32)
            for f in range(1, FIELDS):
                fld = fld + jnp.where(val >= f * width, 1, 0)
            idx[0, r0:r0 + 8, c0:c0 + 128] = val - fld * width
            idx[1, r0:r0 + 8, c0:c0 + 128] = lax.shift_left(jnp.ones((8, 128), I32), fld * FIELD_BITS)
    first = lanes_of(ext[0:targets // 128, :])
    nf[:, 0:targets] = jnp.where(iota((nf.shape[0], targets), 0) == first, 1.0, 0.0).astype(BF16)

    for cp in asks:
        cp.wait_recv()
    lane = iota((1, 128), 1)
    want = jnp.where(lane < HALO, ask_in[0, 0:1, :], ask_in[1, 0:1, :])
    pick = jnp.where(iota((store, 128), 0) == want, 1.0, 0.0).astype(BF16)
    loads[0].wait()
    out = dot(x_ref[...], pick)
    top = out[0:hrows]
    bot = jnp.concatenate([out[hrows:feat], jnp.zeros((2 * hrows - feat, 128), F32)], axis=0)
    low = iota((hrows, 128), 1) < HALO
    rep[0] = jnp.where(low, top, pltpu.roll(bot, HALO, 1)).astype(BF16)
    rep[1] = jnp.where(low, pltpu.roll(top, HALO, 1), bot).astype(BF16)
    reps = []
    for i, nb in enumerate((right, left)):
        reps.append(pltpu.make_async_remote_copy(rep.at[i], rep_in.at[i], hsend.at[2 + i], hrecv.at[2 + i], device_id=(nb,), device_id_type=MESH))
        reps[-1].start()

    block = 16

    def count_block(b, carry):
        base = pl.multiple_of(b * block, block)
        for c0 in range(0, targets, 256):
            row = iota((block, 256), 0) + base
            tot = jnp.zeros((block, 256), I32)
            for k in range(fan_one):
                tot = tot + jnp.where(row == idx[0, k:k + 1, c0:c0 + 256], idx[1, k:k + 1, c0:c0 + 256], 0)
            acc[pl.ds(base, block), c0:c0 + 256] = tot
        return carry

    lax.fori_loop(0, width // block, count_block, 0)
    for f in range(FIELDS):
        cnt = lax.bitwise_and(lax.shift_right_logical(acc[...], f * FIELD_BITS), (1 << FIELD_BITS) - 1)
        nf[f * width:(f + 1) * width, targets:2 * targets] = cnt.astype(F32).astype(BF16)
    both[...] = dot(x_ref[...], nf[0:store, :])

    small[...] = jnp.full(small.shape, -1, I32)
    small[0:fan_two, 0:seeds] = n2_ref[...]
    small[12:13, 0:seeds] = lab_ref[...]
    m2 = jnp.zeros((targets, 128), F32)
    for k in range(fan_two):
        m2 = m2 + jnp.where(iota((targets, 128), 0) == small[k:k + 1, :], 1.0, 0.0)
    m2 = m2.astype(BF16)

    for cp in reps:
        cp.wait_recv()
    from_l, from_r = rep_in[0].astype(F32), rep_in[1].astype(F32)
    halo = jnp.concatenate([jnp.where(low, from_l, pltpu.roll(from_r, HALO, 1)).astype(BF16),
                            jnp.where(low, pltpu.roll(from_l, HALO, 1), from_r).astype(BF16)], axis=0)
    rows = both[...] + dot(halo[0:feat], nf[store:store + 2 * HALO, :])
    x_t = rows[:, 0:targets].astype(BF16)
    a_t = (rows[:, targets:] * (1.0 / fan_one)).astype(BF16)
    loads[1].wait()
    loads[2].wait()
    z = dot(ws1_ref[...], x_t, 0, 0) + dot(wn1_ref[...], a_t, 0, 0)
    z_ref[...] = z
    h = jnp.maximum(z, 0.0).astype(BF16)
    a2 = (dot(h, m2) * (1.0 / fan_two)).astype(BF16)
    hs = h[:, 0:128]
    ws2, wn2 = ws2_ref[...], wn2_ref[...]
    logits = dot(ws2, hs) + dot(wn2, a2)
    shifted = logits - jnp.max(logits, axis=0, keepdims=True)
    log_prob = shifted - jnp.log(jnp.sum(jnp.exp(shifted), axis=0, keepdims=True))
    hit = iota(logits.shape, 0) == small[12:13, :]
    loss = -jnp.sum(jnp.where(hit, log_prob, 0.0))
    gl = (jnp.exp(log_prob) - jnp.where(hit, 1.0, 0.0)) * scale
    gpad[...] = jnp.zeros(gpad.shape, F32)
    gpad[0:classes, :] = jnp.where(lane < seeds, gl, 0.0)
    gb = gpad[...].astype(BF16)
    d_s2 = dot(gb, hs, 1, 1)
    d_n2 = dot(gb, a2, 1, 1)
    d_s2 = jnp.where(iota(d_s2.shape, 0) == classes, loss, d_s2)
    gc = gb[0:classes]
    g_seed = dot(ws2, gc, 0, 0)
    g_agg = dot(wn2, gc, 0, 0) * (1.0 / fan_two)
    p0 = g_agg.astype(BF16)
    r1 = g_agg - p0.astype(F32)
    p1 = r1.astype(BF16)
    p2 = (r1 - p1.astype(F32)).astype(BF16)
    d_h = dot(p0, m2, 1, 1) + (dot(p1, m2, 1, 1) + dot(p2, m2, 1, 1))
    d_h = d_h + jnp.concatenate([g_seed, jnp.zeros((g_seed.shape[0], targets - 128), F32)], axis=1)
    d_z = jnp.where(z_ref[...] > 0, d_h, 0.0).astype(BF16)
    tail = jnp.zeros((2 * hrows - feat, d_z.shape[0]), F32)
    at = 0
    for mat in (jnp.concatenate([dot(x_t, d_z, 1, 1), tail], axis=0),
                jnp.concatenate([dot(a_t, d_z, 1, 1), tail], axis=0), d_s2, d_n2):
        n = mat.shape[0] // 8
        for c0 in range(0, mat.shape[1], 128):
            g[at:at + n] = mat[:, c0:c0 + 128].reshape(n, 8, 128)
            at += n
    if at < g.shape[0]:
        g[at:] = jnp.zeros((g.shape[0] - at, 8, 128), F32)

    copies = []

    def put(src, dst, to):
        k = len(copies)
        cp = pltpu.make_async_remote_copy(src, dst, send.at[k], recv.at[k], device_id=(to,), device_id_type=MESH)
        cp.start()
        copies.append(cp)
        return cp

    other, mine = (1 - core) * half, core * half
    part_a = (nx, xs, xdev, cx, 0, ny, ys, ydev, ca, l1a, w2a, l2a)
    part_b = (ny, ys, ydev, cy, off_b, nx, xs, xdev, cb, l1b, w2b, l2b)
    parts = (part_a, part_b)
    pieces = []
    for i in range(max(nx, ny)):
        for w, p in enumerate(parts):
            if i < p[0]:
                d = (i + 1) % p[0]
                pieces.append((w, d, p[4] + p[1][d] * p[3]))
    arrive = [put(g.at[pl.ds(other + o, parts[w][3])], rc.at[pl.ds(o, parts[w][3])], mate) for w, d, o in pieces]
    first_in = [{}, {}]
    for (w, d, o), cp in zip(pieces, arrive):
        _, _, to, n, _, n2, sub, _, c, land, _, _ = parts[w]
        cp.wait_recv()
        part[pl.ds(o, n)] = g[pl.ds(mine + o, n)] + rc[pl.ds(o, n)]
        if d:
            for i in range(n2):
                e = (i + 1) % n2
                first_in[w][d, e] = put(part.at[pl.ds(o + sub[e] * c, c)], land.at[d - 1, e], to[d])
    second_in, sums = [[], []], [None, None]
    for i in range(max(nx, ny)):
        for w, (n1, own, _, n, off, n2, sub, to, c, land, w2, l2) in enumerate(parts):
            if i < n2:
                e = (i + 1) % n2
                tot = part[pl.ds(off + own[0] * n + sub[e] * c, c)]
                for d in range(1, n1):
                    first_in[w][d, e].wait_recv()
                    tot = tot + land[d - 1, e]
                if e:
                    w2[e - 1] = tot
                    second_in[w].append(put(w2.at[e - 1], l2.at[e - 1], to[e]))
                else:
                    sums[w] = tot
    for w, at, n in ((0, 0, ca), (1, ca, cb)):
        tot = sums[w]
        for e, cp in enumerate(second_in[w]):
            cp.wait_recv()
            tot = tot + parts[w][11][e]
        zc[at:at + n] = tot
    quarter = lax.rem(mz, nq)
    in_z = [put(zc.at[pl.ds((zn * lax.rem(zs[d], nq)) // nq, zsize)], lz.at[mz], zdev[d]) for d in range(1, nz)]
    lz[mz] = zc[pl.ds((zn * quarter) // nq, zsize)]
    for cp in in_z:
        cp.wait_recv()
    tot = lz[0]
    for z in range(1, nz):
        tot = tot + lz[z]
    zg[quarter] = tot
    if nq == 4:
        far = lax.rem(mz + 2 + 4 * lax.rem(mz, 2), nz)
        targets_z = (zdev[1], zdev[nz - 1], dev(far, my, mx, core))
        in_z = [put(zg.at[quarter], zg.at[quarter], to) for to in targets_z]
        for cp in in_z:
            cp.wait_recv()
    base = [mine + p[4] + p[1][0] * p[3] for p in parts]
    spots = [base[w] + p[6][0] * p[8] for w, p in enumerate(parts)]
    for q in range(nq):
        lo = (zn * q) // nq
        end = (zn * (q + 1)) // nq
        for t in range(lo, end):
            at = spots[0] + t if t < ca else spots[1] + (t - ca)
            full[pl.ds(at, 1)] = zg[q, t - lo:t - lo + 1]
    back = []

    def spread(w, at):
        n1, _, to, _, _, _, _, _, c, _, _, _ = parts[w]
        got = [put(full.at[pl.ds(at, c)], full.at[pl.ds(at, c)], to[d]) for d in range(1, n1)]
        back.append(put(full.at[pl.ds(at, c)], full.at[pl.ds(at, c)], mate))
        return got

    second_in = [[], []]
    for w, p in enumerate(parts):
        for e in range(1, p[5]):
            second_in[w].append(put(full.at[pl.ds(spots[w], p[8])], full.at[pl.ds(spots[w], p[8])], p[7][e]))
    first_in = [[spread(w, spots[w])] for w in range(2)]
    for i in range(max(nx, ny)):
        for w, (n1, own, _, n, off, n2, sub, _, c, _, _, _) in enumerate(parts):
            if i < n2 - 1:
                second_in[w][i].wait_recv()
                first_in[w].append(spread(w, base[w] + sub[n2 - 1 - i] * c))
    for i in range(max(nx, ny)):
        for w, (n1, own, _, n, off, n2, sub, _, c, _, _, _) in enumerate(parts):
            if i < n2:
                for d in range(1, n1):
                    first_in[w][i][d - 1].wait_recv()
                    at = mine + off + own[n1 - d] * n + sub[(n2 - i) % n2] * c
                    back.append(put(full.at[pl.ds(at, c)], full.at[pl.ds(at, c)], mate))
    for cp in back:
        cp.wait_recv()
    for cp in copies + asks + reps:
        cp.wait_send()
    r_ref[...] = full[...]


def copy_count(group):
    nx, ny, nz = dims_of(group)
    return nx + ny + 2 * ((nx - 1) * ny + (ny - 1) * nx + nx - 1 + ny - 1) + nz - 1 + (3 if nz == 8 else 0) + 2 * nx * ny


def output_kernel(scale, r_ref, loss_ref, s1_ref, n1_ref, s2_ref, n2_ref):
    at = 0
    classes = s2_ref.shape[0]
    for ref in (s1_ref, n1_ref, s2_ref, n2_ref):
        rows, cols = ref.shape
        n = -(-rows // 8)
        for c0 in range(0, cols, 128):
            val = r_ref[at:at + n].reshape(n * 8, 128)
            ref[:, c0:c0 + 128] = val[0:rows]
            if ref is s2_ref and c0 == 0:
                loss_ref[...] = val[classes:classes + 1, 0:1] * scale
            at += n


def solution(mesh):
    group = mesh.shape['g']

    def device_step(x_local, front_ids, nbr_one, nbr_two, labels, w_self1, w_nbr1, w_self2, w_nbr2):
        store, feat = x_local.shape
        targets, fan_one = nbr_one.shape
        seeds = nbr_two.shape[0]
        hidden, classes = w_self2.shape
        frows = -(-feat // 32) * 32
        scale = 1.0 / (group * seeds)
        fid = front_ids.reshape(-1, 128)
        width = -(-(store + 2 * HALO) // (FIELDS * 16)) * 16
        nx, ny, nz = dims_of(group)
        ca, cb = chunks_of(group)
        cx, cy, zn = ny * ca, nx * cb, ca + cb
        nq = max(1, nz // 2)
        zsize = -(-zn // nq)
        half = nx * cx + ny * cy
        total = 2 * half
        n = copy_count(group)
        dma = pltpu.SemaphoreType.DMA

        def buf(*lead):
            return VMEM((*lead, 8, 128), F32)

        vm, hbm = pl.BlockSpec(memory_space=VMEM), pl.BlockSpec(memory_space=pl.ANY)
        sums = pl.pallas_call(
            functools.partial(step_kernel, group, scale),
            name='train_step',
            out_shape=jax.ShapeDtypeStruct((total, 8, 128), F32),
            in_specs=[vm, hbm, vm, vm, vm, hbm, hbm, vm, vm],
            out_specs=vm,
            scratch_shapes=[
                VMEM((feat, store), BF16), VMEM((feat, hidden), BF16), VMEM((feat, hidden), BF16), dma((3,)),
                VMEM((8, 128), I32), VMEM((2, 8, 128), I32), VMEM((2, frows // 2, 128), BF16),
                VMEM((2, frows // 2, 128), BF16), dma((4,)), dma((4,)),
                VMEM((16, 128), I32), VMEM((2, -(-fan_one // 8) * 8, targets), I32), VMEM((width, targets), I32),
                VMEM((FIELDS * width, 2 * targets), BF16), VMEM((feat, 2 * targets), F32), VMEM((hidden, targets), F32),
                VMEM((-(-classes // 16) * 16, 128), F32), buf(total),
                buf(half), buf(half), buf(nx - 1, ny, ca), buf(ny - 1, nx, cb), buf(ny - 1, ca), buf(nx - 1, cb),
                buf(ny - 1, ca), buf(nx - 1, cb), buf(zn), buf(nz, zsize), buf(nq, zsize), buf(total),
                dma((n,)), dma((n,))],
            compiler_params=pltpu.CompilerParams(collective_id=0, has_side_effects=True,
                                                 vmem_limit_bytes=60 * 1024 * 1024),
        )(fid, x_local.T, nbr_one.T, nbr_two.T, labels.reshape(1, -1), w_self1, w_nbr1, w_self2.T, w_nbr2.T)
        loss, d_s1, d_n1, d_s2, d_n2 = pl.pallas_call(
            functools.partial(output_kernel, scale),
            name='split_outputs',
            out_shape=[jax.ShapeDtypeStruct((1, 1), F32), jax.ShapeDtypeStruct((feat, hidden), F32),
                       jax.ShapeDtypeStruct((feat, hidden), F32), jax.ShapeDtypeStruct((classes, hidden), F32),
                       jax.ShapeDtypeStruct((classes, hidden), F32)],
            in_specs=[vm], out_specs=[vm] * 5,
        )(sums)
        return loss[0, 0], d_s1, d_n1, d_s2.T, d_n2.T

    return jax.shard_map(device_step, mesh=mesh,
                         in_specs=(P('g', None), P('g'), P('g', None), P('g', None), P('g'), P(), P(), P(), P()),
                         out_specs=(P(), P(), P(), P(), P()), check_vma=False)
```

```python
import functools

import jax
import jax.numpy as jnp
from jax import lax
from jax.experimental import pallas as pl
from jax.experimental.pallas import tpu as pltpu
from jax.sharding import PartitionSpec as P

MESH = pl.DeviceIdType.MESH
F32, BF16, I32 = jnp.float32, jnp.bfloat16, jnp.int32
VMEM = pltpu.VMEM

HALO = 64
FIELDS, FIELD_BITS = 6, 5


def dims_of(group):
    return {256: (4, 4, 8), 16: (2, 2, 2)}[group]


def chunks_of(group):
    return {256: (6, 5), 16: (21, 20)}[group]


def dot(a, b, ca=1, cb=0):
    return lax.dot_general(a, b, (((ca,), (cb,)), ((), ())), preferred_element_type=F32)


def iota(shape, dim):
    return lax.broadcasted_iota(I32, shape, dim)


def frontier_ext(fid, me, group, rows_log2):
    store = 1 << rows_log2
    owner = lax.shift_right_logical(fid, rows_log2)
    off = lax.bitwise_and(fid, store - 1)
    left, right = lax.rem(me + group - 1, group), lax.rem(me + 1, group)
    is_l, is_r = owner == left, owner == right
    mask = jnp.concatenate([jnp.where(is_l, 1.0, 0.0), jnp.where(is_r, 1.0, 0.0)], axis=0).astype(BF16)
    n = fid.shape[0]
    upper = jnp.where(iota((128, 128), 0) < iota((128, 128), 1), 1.0, 0.0).astype(BF16)
    ri, ci = iota((2 * n, 2 * n), 0), iota((2 * n, 2 * n), 1)
    before = jnp.where((ci < ri) & ((ci < n) == (ri < n)), 1.0, 0.0).astype(BF16)
    ones = jnp.ones((128, 128), BF16)
    rank = dot(mask, upper) + dot(dot(before, mask).astype(BF16), ones)
    rank = rank.astype(I32)
    rank_l, rank_r = rank[:n], rank[n:]
    ext = jnp.where(is_l, store + rank_l, jnp.where(is_r, store + HALO + rank_r, off))
    return ext, off


def lanes_of(a):
    return jnp.concatenate([a[i:i + 1, :] for i in range(a.shape[0])], axis=1)


def ask_rows(ext, off, store):
    key = lanes_of(ext) - store
    offs = lanes_of(off)
    pick = jnp.where(iota((2 * HALO, key.shape[1]), 0) == key, 1.0, 0.0).astype(BF16)
    row = iota((16, key.shape[1]), 0)
    hi, lo = lax.shift_right_logical(offs, 6), lax.bitwise_and(offs, 63)
    parts = jnp.where(row == 0, hi, jnp.where(row == 1, lo, 0)).astype(F32).astype(BF16)
    got = dot(parts, pick, 1, 1).astype(I32)
    return got[0:1] * 64 + got[1:2]


def step_kernel(group, scale, fid_hbm, x_hbm, n1_hbm, n2_hbm, lab_hbm, ws1_hbm, wn1_hbm, ws2_hbm, wn2_hbm, r_ref,
                fid_ref, x_ref, n1_ref, n2_ref, lab_ref, ws1_ref, wn1_ref, ws2_ref, wn2_ref, in_sem,
                ws1_t, wn1_t, ws2_t, wn2_t, ask, ask_in, rep, rep_in, hsend, hrecv,
                small, idx, acc, nf, both, z_ref, gpad, g,
                rc, part, l1a, l1b, w2a, w2b, l2a, l2b, zc, lz, zg, full, send, recv):
    nx, ny, nz = dims_of(group)
    ca, cb = chunks_of(group)
    cx, cy, zn = ny * ca, nx * cb, ca + cb
    nq = max(1, nz // 2)
    zsize = -(-zn // nq)
    off_b = nx * cx
    half = off_b + ny * cy
    me = lax.axis_index('g')
    core = lax.rem(me, 2)
    mx = lax.rem(me // 2, nx)
    my = lax.rem(me // (2 * nx), ny)
    mz = me // (2 * nx * ny)

    def dev(z, y, x, c):
        return ((z * ny + y) * nx + x) * 2 + c

    mate = dev(mz, my, mx, 1 - core)
    xs = [lax.rem(mx + d, nx) for d in range(nx)]
    ys = [lax.rem(my + d, ny) for d in range(ny)]
    zs = [lax.rem(mz + d, nz) for d in range(nz)]
    xdev = [dev(mz, my, x, core) for x in xs]
    ydev = [dev(mz, y, mx, core) for y in ys]
    zdev = [dev(z, my, mx, core) for z in zs]
    left, right = lax.rem(me + group - 1, group), lax.rem(me + 1, group)

    barrier = pltpu.get_barrier_semaphore()
    peers = [left, right, mate] + xdev[1:] + ydev[1:] + zdev[1:]
    for nb in peers:
        pl.semaphore_signal(barrier, inc=1, device_id=(nb,), device_id_type=MESH)
    loads = [pltpu.make_async_copy(src, dst, in_sem.at[i]) for i, (src, dst) in
             enumerate(((fid_hbm, fid_ref), (n1_hbm, n1_ref), (x_hbm, x_ref), (n2_hbm, n2_ref), (lab_hbm, lab_ref),
                        (ws1_hbm, ws1_ref), (wn1_hbm, wn1_ref), (ws2_hbm, ws2_ref), (wn2_hbm, wn2_ref)))]
    for cp in loads:
        cp.start()

    feat, store = x_ref.shape
    targets = n1_ref.shape[1]
    fan_one = n1_ref.shape[0]
    fan_two, seeds = n2_ref.shape
    classes = ws2_ref.shape[0]
    width = acc.shape[0]
    hrows = rep.shape[1]
    loads[0].wait()
    ext, off = frontier_ext(fid_ref[...], me, group, store.bit_length() - 1)
    ask[...] = jnp.broadcast_to(ask_rows(ext, off, store), ask.shape)
    pl.semaphore_wait(barrier, len(peers))
    asks = []
    for i, nb in enumerate((left, right)):
        asks.append(pltpu.make_async_remote_copy(ask, ask_in.at[i], hsend.at[i], hrecv.at[i], device_id=(nb,), device_id_type=MESH))
        asks[-1].start()

    loads[1].wait()
    for r0 in range(0, fan_one, 8):
        nr = min(8, fan_one - r0)
        for c0 in range(0, targets, 128):
            pos = n1_ref[r0:r0 + nr, c0:c0 + 128]
            if nr < 8:
                pos = jnp.broadcast_to(pos[0:1], (8, 128)) if nr == 1 else jnp.concatenate([pos, pos[0:8 - nr]], axis=0)
            hi = lax.shift_right_logical(pos, 7)
            lo = lax.bitwise_and(pos, 127)
            val = jnp.zeros((8, 128), I32)
            for h in range(ext.shape[0]):
                row = jnp.broadcast_to(ext[h:h + 1, :], (8, 128))
                val = jnp.where(hi == h, jnp.take_along_axis(row, lo, axis=1, mode='promise_in_bounds'), val)
            fld = jnp.zeros((8, 128), I32)
            for f in range(1, FIELDS):
                fld = fld + jnp.where(val >= f * width, 1, 0)
            idx[0, r0:r0 + 8, c0:c0 + 128] = val - fld * width
            idx[1, r0:r0 + 8, c0:c0 + 128] = lax.shift_left(jnp.ones((8, 128), I32), fld * FIELD_BITS)
    first = lanes_of(ext[0:targets // 128, :])
    nf[:, 0:targets] = jnp.where(iota((nf.shape[0], targets), 0) == first, 1.0, 0.0).astype(BF16)

    for cp in asks:
        cp.wait_recv()
    lane = iota((1, 128), 1)
    want = jnp.where(lane < HALO, ask_in[0, 0:1, :], ask_in[1, 0:1, :])
    pick = jnp.where(iota((store, 128), 0) == want, 1.0, 0.0).astype(BF16)
    loads[2].wait()
    out = dot(x_ref[...], pick)
    top = out[0:hrows]
    bot = jnp.concatenate([out[hrows:feat], jnp.zeros((2 * hrows - feat, 128), F32)], axis=0)
    low = iota((hrows, 128), 1) < HALO
    rep[0] = jnp.where(low, top, pltpu.roll(bot, HALO, 1)).astype(BF16)
    rep[1] = jnp.where(low, pltpu.roll(top, HALO, 1), bot).astype(BF16)
    reps = []
    for i, nb in enumerate((right, left)):
        reps.append(pltpu.make_async_remote_copy(rep.at[i], rep_in.at[i], hsend.at[2 + i], hrecv.at[2 + i], device_id=(nb,), device_id_type=MESH))
        reps[-1].start()

    block = 16

    def count_block(b, carry):
        base = pl.multiple_of(b * block, block)
        for c0 in range(0, targets, 256):
            row = iota((block, 256), 0) + base
            tot = jnp.zeros((block, 256), I32)
            for k in range(fan_one):
                tot = tot + jnp.where(row == idx[0, k:k + 1, c0:c0 + 256], idx[1, k:k + 1, c0:c0 + 256], 0)
            acc[pl.ds(base, block), c0:c0 + 256] = tot
        return carry

    lax.fori_loop(0, width // block, count_block, 0)
    for f in range(FIELDS):
        cnt = lax.bitwise_and(lax.shift_right_logical(acc[...], f * FIELD_BITS), (1 << FIELD_BITS) - 1)
        nf[f * width:(f + 1) * width, targets:2 * targets] = cnt.astype(F32).astype(BF16)
    both[...] = dot(x_ref[...], nf[0:store, :])

    for cp in loads[3:]:
        cp.wait()
    small[...] = jnp.full(small.shape, -1, I32)
    small[0:fan_two, 0:seeds] = n2_ref[...]
    small[12:13, 0:seeds] = lab_ref[...]
    m2 = jnp.zeros((targets, 128), F32)
    for k in range(fan_two):
        m2 = m2 + jnp.where(iota((targets, 128), 0) == small[k:k + 1, :], 1.0, 0.0)
    m2 = m2.astype(BF16)
    for src, dst in ((ws1_ref, ws1_t), (wn1_ref, wn1_t), (ws2_ref, ws2_t), (wn2_ref, wn2_t)):
        dst[...] = src[...].T

    for cp in reps:
        cp.wait_recv()
    from_l, from_r = rep_in[0].astype(F32), rep_in[1].astype(F32)
    halo = jnp.concatenate([jnp.where(low, from_l, pltpu.roll(from_r, HALO, 1)).astype(BF16),
                            jnp.where(low, pltpu.roll(from_l, HALO, 1), from_r).astype(BF16)], axis=0)
    rows = both[...] + dot(halo[0:feat], nf[store:store + 2 * HALO, :])
    x_t = rows[:, 0:targets].astype(BF16)
    a_t = (rows[:, targets:] * (1.0 / fan_one)).astype(BF16)
    z = dot(ws1_t[...], x_t) + dot(wn1_t[...], a_t)
    z_ref[...] = z
    h = jnp.maximum(z, 0.0).astype(BF16)
    a2 = (dot(h, m2) * (1.0 / fan_two)).astype(BF16)
    hs = h[:, 0:128]
    ws2, wn2 = ws2_ref[...], wn2_ref[...]
    logits = dot(ws2, hs) + dot(wn2, a2)
    shifted = logits - jnp.max(logits, axis=0, keepdims=True)
    log_prob = shifted - jnp.log(jnp.sum(jnp.exp(shifted), axis=0, keepdims=True))
    hit = iota(logits.shape, 0) == small[12:13, :]
    loss = -jnp.sum(jnp.where(hit, log_prob, 0.0))
    gl = (jnp.exp(log_prob) - jnp.where(hit, 1.0, 0.0)) * scale
    gpad[...] = jnp.zeros(gpad.shape, F32)
    gpad[0:classes, :] = jnp.where(lane < seeds, gl, 0.0)
    gb = gpad[...].astype(BF16)
    d_s2 = dot(gb, hs, 1, 1)
    d_n2 = dot(gb, a2, 1, 1)
    d_s2 = jnp.where(iota(d_s2.shape, 0) == classes, loss, d_s2)
    gc = gb[0:classes]
    g_seed = dot(ws2_t[...], gc)
    g_agg = dot(wn2_t[...], gc) * (1.0 / fan_two)
    p0 = g_agg.astype(BF16)
    r1 = g_agg - p0.astype(F32)
    p1 = r1.astype(BF16)
    p2 = (r1 - p1.astype(F32)).astype(BF16)
    d_h = dot(p0, m2, 1, 1) + (dot(p1, m2, 1, 1) + dot(p2, m2, 1, 1))
    d_h = d_h + jnp.concatenate([g_seed, jnp.zeros((g_seed.shape[0], targets - 128), F32)], axis=1)
    d_z = jnp.where(z_ref[...] > 0, d_h, 0.0).astype(BF16)
    tail = jnp.zeros((2 * hrows - feat, d_z.shape[0]), F32)
    at = 0
    for mat in (jnp.concatenate([dot(x_t, d_z, 1, 1), tail], axis=0),
                jnp.concatenate([dot(a_t, d_z, 1, 1), tail], axis=0), d_s2, d_n2):
        n = mat.shape[0] // 8
        for c0 in range(0, mat.shape[1], 128):
            g[at:at + n] = mat[:, c0:c0 + 128].reshape(n, 8, 128)
            at += n
    if at < g.shape[0]:
        g[at:] = jnp.zeros((g.shape[0] - at, 8, 128), F32)

    copies = []

    def put(src, dst, to):
        k = len(copies)
        cp = pltpu.make_async_remote_copy(src, dst, send.at[k], recv.at[k], device_id=(to,), device_id_type=MESH)
        cp.start()
        copies.append(cp)
        return cp

    other, mine = (1 - core) * half, core * half
    part_a = (nx, xs, xdev, cx, 0, ny, ys, ydev, ca, l1a, w2a, l2a)
    part_b = (ny, ys, ydev, cy, off_b, nx, xs, xdev, cb, l1b, w2b, l2b)
    parts = (part_a, part_b)
    pieces = []
    for i in range(max(nx, ny)):
        for w, p in enumerate(parts):
            if i < p[0]:
                d = (i + 1) % p[0]
                pieces.append((w, d, p[4] + p[1][d] * p[3]))
    arrive = [put(g.at[pl.ds(other + o, parts[w][3])], rc.at[pl.ds(o, parts[w][3])], mate) for w, d, o in pieces]
    first_in = [{}, {}]
    for (w, d, o), cp in zip(pieces, arrive):
        _, _, to, n, _, n2, sub, _, c, land, _, _ = parts[w]
        cp.wait_recv()
        part[pl.ds(o, n)] = g[pl.ds(mine + o, n)] + rc[pl.ds(o, n)]
        if d:
            for i in range(n2):
                e = (i + 1) % n2
                first_in[w][d, e] = put(part.at[pl.ds(o + sub[e] * c, c)], land.at[d - 1, e], to[d])
    second_in, sums = [[], []], [None, None]
    for i in range(max(nx, ny)):
        for w, (n1, own, _, n, off, n2, sub, to, c, land, w2, l2) in enumerate(parts):
            if i < n2:
                e = (i + 1) % n2
                tot = part[pl.ds(off + own[0] * n + sub[e] * c, c)]
                for d in range(1, n1):
                    first_in[w][d, e].wait_recv()
                    tot = tot + land[d - 1, e]
                if e:
                    w2[e - 1] = tot
                    second_in[w].append(put(w2.at[e - 1], l2.at[e - 1], to[e]))
                else:
                    sums[w] = tot
    for w, at, n in ((0, 0, ca), (1, ca, cb)):
        tot = sums[w]
        for e, cp in enumerate(second_in[w]):
            cp.wait_recv()
            tot = tot + parts[w][11][e]
        zc[at:at + n] = tot
    quarter = lax.rem(mz, nq)
    in_z = [put(zc.at[pl.ds((zn * lax.rem(zs[d], nq)) // nq, zsize)], lz.at[mz], zdev[d]) for d in range(1, nz)]
    lz[mz] = zc[pl.ds((zn * quarter) // nq, zsize)]
    for cp in in_z:
        cp.wait_recv()
    tot = lz[0]
    for z in range(1, nz):
        tot = tot + lz[z]
    zg[quarter] = tot
    if nq == 4:
        far = lax.rem(mz + 2 + 4 * lax.rem(mz, 2), nz)
        targets_z = (zdev[1], zdev[nz - 1], dev(far, my, mx, core))
        in_z = [put(zg.at[quarter], zg.at[quarter], to) for to in targets_z]
        for cp in in_z:
            cp.wait_recv()
    base = [mine + p[4] + p[1][0] * p[3] for p in parts]
    spots = [base[w] + p[6][0] * p[8] for w, p in enumerate(parts)]
    for q in range(nq):
        lo = (zn * q) // nq
        end = (zn * (q + 1)) // nq
        for t in range(lo, end):
            at = spots[0] + t if t < ca else spots[1] + (t - ca)
            full[pl.ds(at, 1)] = zg[q, t - lo:t - lo + 1]
    back = []

    def spread(w, at):
        n1, _, to, _, _, _, _, _, c, _, _, _ = parts[w]
        got = [put(full.at[pl.ds(at, c)], full.at[pl.ds(at, c)], to[d]) for d in range(1, n1)]
        back.append(put(full.at[pl.ds(at, c)], full.at[pl.ds(at, c)], mate))
        return got

    second_in = [[], []]
    for w, p in enumerate(parts):
        for e in range(1, p[5]):
            second_in[w].append(put(full.at[pl.ds(spots[w], p[8])], full.at[pl.ds(spots[w], p[8])], p[7][e]))
    first_in = [[spread(w, spots[w])] for w in range(2)]
    for i in range(max(nx, ny)):
        for w, (n1, own, _, n, off, n2, sub, _, c, _, _, _) in enumerate(parts):
            if i < n2 - 1:
                second_in[w][i].wait_recv()
                first_in[w].append(spread(w, base[w] + sub[n2 - 1 - i] * c))
    for i in range(max(nx, ny)):
        for w, (n1, own, _, n, off, n2, sub, _, c, _, _, _) in enumerate(parts):
            if i < n2:
                for d in range(1, n1):
                    first_in[w][i][d - 1].wait_recv()
                    at = mine + off + own[n1 - d] * n + sub[(n2 - i) % n2] * c
                    back.append(put(full.at[pl.ds(at, c)], full.at[pl.ds(at, c)], mate))
    for cp in back:
        cp.wait_recv()
    for cp in copies + asks + reps:
        cp.wait_send()
    r_ref[...] = full[...]


def copy_count(group):
    nx, ny, nz = dims_of(group)
    return nx + ny + 2 * ((nx - 1) * ny + (ny - 1) * nx + nx - 1 + ny - 1) + nz - 1 + (3 if nz == 8 else 0) + 2 * nx * ny


def output_kernel(scale, r_ref, loss_ref, s1_hbm, n1_hbm, s2_hbm, n2_hbm, s1, n1, s2, n2, sem):
    at, k = 0, 0
    classes = s2.shape[0]
    copies = []
    for ref, hbm in ((s1, s1_hbm), (n1, n1_hbm), (s2, s2_hbm), (n2, n2_hbm)):
        rows, cols = ref.shape
        n = -(-rows // 8)
        step = n if n < 16 else 19
        for r0 in range(0, n, step):
            lo, hi = r0 * 8, min(rows, (r0 + step) * 8)
            for c in range(cols // 128):
                val = r_ref[at + c * n + r0:at + c * n + r0 + step].reshape(step * 8, 128)
                ref[lo:hi, c * 128:(c + 1) * 128] = val[0:hi - lo]
                if ref is s2 and c == 0:
                    loss_ref[...] = val[classes:classes + 1, 0:1] * scale
            cp = pltpu.make_async_copy(ref.at[lo:hi], hbm.at[lo:hi], sem.at[k])
            cp.start()
            copies.append(cp)
            k += 1
        at += n * (cols // 128)
    for cp in copies:
        cp.wait()


def solution(mesh):
    group = mesh.shape['g']

    def device_step(x_local, front_ids, nbr_one, nbr_two, labels, w_self1, w_nbr1, w_self2, w_nbr2):
        store, feat = x_local.shape
        targets, fan_one = nbr_one.shape
        seeds, fan_two = nbr_two.shape
        hidden, classes = w_self2.shape
        frows = -(-feat // 32) * 32
        scale = 1.0 / (group * seeds)
        fid = front_ids.reshape(-1, 128)
        width = -(-(store + 2 * HALO) // (FIELDS * 16)) * 16
        nx, ny, nz = dims_of(group)
        ca, cb = chunks_of(group)
        cx, cy, zn = ny * ca, nx * cb, ca + cb
        nq = max(1, nz // 2)
        zsize = -(-zn // nq)
        half = nx * cx + ny * cy
        total = 2 * half
        n = copy_count(group)
        dma = pltpu.SemaphoreType.DMA

        def buf(*lead):
            return VMEM((*lead, 8, 128), F32)

        vm, hbm = pl.BlockSpec(memory_space=VMEM), pl.BlockSpec(memory_space=pl.ANY)
        sums = pl.pallas_call(
            functools.partial(step_kernel, group, scale),
            name='train_step',
            out_shape=VMEM((total, 8, 128), F32),
            in_specs=[hbm] * 9,
            out_specs=vm,
            scratch_shapes=[
                VMEM(fid.shape, I32), VMEM((feat, store), BF16), VMEM((fan_one, targets), I32), VMEM((fan_two, seeds), I32),
                VMEM((1, seeds), I32), VMEM((feat, hidden), BF16), VMEM((feat, hidden), BF16), VMEM((classes, hidden), BF16),
                VMEM((classes, hidden), BF16), dma((9,)),
                VMEM((hidden, feat), BF16), VMEM((hidden, feat), BF16), VMEM((hidden, classes), BF16), VMEM((hidden, classes), BF16),
                VMEM((8, 128), I32), VMEM((2, 8, 128), I32), VMEM((2, frows // 2, 128), BF16),
                VMEM((2, frows // 2, 128), BF16), dma((4,)), dma((4,)),
                VMEM((16, 128), I32), VMEM((2, -(-fan_one // 8) * 8, targets), I32), VMEM((width, targets), I32),
                VMEM((FIELDS * width, 2 * targets), BF16), VMEM((feat, 2 * targets), F32), VMEM((hidden, targets), F32),
                VMEM((-(-classes // 16) * 16, 128), F32), buf(total),
                buf(half), buf(half), buf(nx - 1, ny, ca), buf(ny - 1, nx, cb), buf(ny - 1, ca), buf(nx - 1, cb),
                buf(ny - 1, ca), buf(nx - 1, cb), buf(zn), buf(nz, zsize), buf(nq, zsize), buf(total),
                dma((n,)), dma((n,))],
            compiler_params=pltpu.CompilerParams(collective_id=0, has_side_effects=True,
                                                 vmem_limit_bytes=60 * 1024 * 1024),
        )(fid, x_local.T, nbr_one.T, nbr_two.T, labels.reshape(1, -1), w_self1, w_nbr1, w_self2.T, w_nbr2.T)
        loss, d_s1, d_n1, d_s2, d_n2 = pl.pallas_call(
            functools.partial(output_kernel, scale),
            name='split_outputs',
            out_shape=[jax.ShapeDtypeStruct((1, 1), F32), jax.ShapeDtypeStruct((feat, hidden), F32),
                       jax.ShapeDtypeStruct((feat, hidden), F32), jax.ShapeDtypeStruct((classes, hidden), F32),
                       jax.ShapeDtypeStruct((classes, hidden), F32)],
            in_specs=[vm], out_specs=[vm] + [hbm] * 4,
            scratch_shapes=[VMEM((feat, hidden), F32), VMEM((feat, hidden), F32), VMEM((classes, hidden), F32),
                            VMEM((classes, hidden), F32), dma((10,))],
        )(pltpu.with_memory_space_constraint(sums, VMEM))
        return loss[0, 0], d_s1, d_n1, d_s2.T, d_n2.T

    return jax.shard_map(device_step, mesh=mesh,
                         in_specs=(P('g', None), P('g'), P('g', None), P('g', None), P('g'), P(), P(), P(), P()),
                         out_specs=(P(), P(), P(), P(), P()), check_vma=False)
```

```python
import functools

import jax
import jax.numpy as jnp
from jax import lax
from jax.experimental import pallas as pl
from jax.experimental.pallas import tpu as pltpu
from jax.sharding import PartitionSpec as P

MESH = pl.DeviceIdType.MESH
F32, BF16, I32 = jnp.float32, jnp.bfloat16, jnp.int32
VMEM = pltpu.VMEM

HALO = 64
FIELDS, FIELD_BITS = 6, 5


def dims_of(group):
    return {256: (4, 4, 8), 16: (2, 2, 2)}[group]


def chunks_of(group):
    return {256: (6, 5), 16: (21, 20)}[group]


def dot(a, b, ca=1, cb=0):
    return lax.dot_general(a, b, (((ca,), (cb,)), ((), ())), preferred_element_type=F32)


def iota(shape, dim):
    return lax.broadcasted_iota(I32, shape, dim)


def frontier_ext(fid, me, group, rows_log2):
    store = 1 << rows_log2
    owner = lax.shift_right_logical(fid, rows_log2)
    off = lax.bitwise_and(fid, store - 1)
    left, right = lax.rem(me + group - 1, group), lax.rem(me + 1, group)
    is_l, is_r = owner == left, owner == right
    mask = jnp.concatenate([jnp.where(is_l, 1.0, 0.0), jnp.where(is_r, 1.0, 0.0)], axis=0).astype(BF16)
    n = fid.shape[0]
    upper = jnp.where(iota((128, 128), 0) < iota((128, 128), 1), 1.0, 0.0).astype(BF16)
    ri, ci = iota((2 * n, 2 * n), 0), iota((2 * n, 2 * n), 1)
    before = jnp.where((ci < ri) & ((ci < n) == (ri < n)), 1.0, 0.0).astype(BF16)
    ones = jnp.ones((128, 128), BF16)
    rank = dot(mask, upper) + dot(dot(before, mask).astype(BF16), ones)
    rank = rank.astype(I32)
    rank_l, rank_r = rank[:n], rank[n:]
    ext = jnp.where(is_l, store + rank_l, jnp.where(is_r, store + HALO + rank_r, off))
    return ext, off


def lanes_of(a):
    return jnp.concatenate([a[i:i + 1, :] for i in range(a.shape[0])], axis=1)


def ask_rows(ext, off, store):
    key = lanes_of(ext) - store
    offs = lanes_of(off)
    pick = jnp.where(iota((2 * HALO, key.shape[1]), 0) == key, 1.0, 0.0).astype(BF16)
    row = iota((16, key.shape[1]), 0)
    hi, lo = lax.shift_right_logical(offs, 6), lax.bitwise_and(offs, 63)
    parts = jnp.where(row == 0, hi, jnp.where(row == 1, lo, 0)).astype(F32).astype(BF16)
    got = dot(parts, pick, 1, 1).astype(I32)
    return got[0:1] * 64 + got[1:2]


def step_kernel(group, scale, fid_hbm, x_hbm, n1_hbm, n2_hbm, lab_hbm, ws1_hbm, wn1_hbm, ws2_hbm, wn2_hbm, r_ref,
                fid_ref, x_ref, n1_ref, n2_ref, lab_ref, ws1_ref, wn1_ref, ws2_ref, wn2_ref, in_sem,
                ws1_t, wn1_t, ws2_t, wn2_t, ask, ask_in, rep, rep_in, hsend, hrecv, up,
                small, idx, acc, nf, both, z_ref, gpad, g,
                rc, part, l1a, l1b, w2a, w2b, l2a, l2b, zc, lz, zg, send, recv):
    nx, ny, nz = dims_of(group)
    ca, cb = chunks_of(group)
    cx, cy, zn = ny * ca, nx * cb, ca + cb
    nq = max(1, nz // 2)
    zsize = -(-zn // nq)
    off_b = nx * cx
    half = off_b + ny * cy
    me = lax.axis_index('g')
    core = lax.rem(me, 2)
    mx = lax.rem(me // 2, nx)
    my = lax.rem(me // (2 * nx), ny)
    mz = me // (2 * nx * ny)

    def dev(z, y, x, c):
        return ((z * ny + y) * nx + x) * 2 + c

    mate = dev(mz, my, mx, 1 - core)
    xs = [lax.rem(mx + d, nx) for d in range(nx)]
    ys = [lax.rem(my + d, ny) for d in range(ny)]
    zs = [lax.rem(mz + d, nz) for d in range(nz)]
    xdev = [dev(mz, my, x, core) for x in xs]
    ydev = [dev(mz, y, mx, core) for y in ys]
    zdev = [dev(z, my, mx, core) for z in zs]
    left, right = lax.rem(me + group - 1, group), lax.rem(me + 1, group)

    barrier = pltpu.get_barrier_semaphore()
    peers = [left, right, mate] + xdev[1:] + ydev[1:]

    def signal(sem, to):
        pl.semaphore_signal(sem, inc=1, device_id=(to,), device_id_type=MESH)

    for nb in peers:
        pl.semaphore_signal(barrier, inc=1, device_id=(nb,), device_id_type=MESH)
    for d in range(1, nz):
        pl.when(mz + d < nz)(functools.partial(signal, barrier, zdev[d]))
    loads = [pltpu.make_async_copy(src, dst, in_sem.at[i]) for i, (src, dst) in
             enumerate(((fid_hbm, fid_ref), (n1_hbm, n1_ref), (x_hbm, x_ref), (n2_hbm, n2_ref), (lab_hbm, lab_ref),
                        (ws1_hbm, ws1_ref), (wn1_hbm, wn1_ref), (ws2_hbm, ws2_ref), (wn2_hbm, wn2_ref)))]
    for cp in loads:
        cp.start()

    feat, store = x_ref.shape
    targets = n1_ref.shape[1]
    fan_one = n1_ref.shape[0]
    fan_two, seeds = n2_ref.shape
    classes = ws2_ref.shape[0]
    width = acc.shape[0]
    hrows = rep.shape[1]
    loads[0].wait()
    ext, off = frontier_ext(fid_ref[...], me, group, store.bit_length() - 1)
    ask[...] = jnp.broadcast_to(ask_rows(ext, off, store), ask.shape)
    asks = []
    for i, nb in enumerate((left, right)):
        asks.append(pltpu.make_async_remote_copy(ask, ask_in.at[i], hsend.at[i], hrecv.at[i], device_id=(nb,), device_id_type=MESH))

    def ask_neighbours():
        pl.semaphore_wait(barrier, len(peers) + mz)
        for cp in asks:
            cp.start()
        for d in range(1, nz):
            pl.when(mz + d >= nz)(functools.partial(signal, up.at[nz - d], zdev[d]))

    first_of_plane = lax.rem(me, 2 * nx * ny) == 0
    pl.when(jnp.logical_not(first_of_plane))(ask_neighbours)

    loads[1].wait()
    for r0 in range(0, fan_one, 8):
        nr = min(8, fan_one - r0)
        for c0 in range(0, targets, 128):
            pos = n1_ref[r0:r0 + nr, c0:c0 + 128]
            if nr < 8:
                pos = jnp.broadcast_to(pos[0:1], (8, 128)) if nr == 1 else jnp.concatenate([pos, pos[0:8 - nr]], axis=0)
            hi = lax.shift_right_logical(pos, 7)
            lo = lax.bitwise_and(pos, 127)
            val = jnp.zeros((8, 128), I32)
            for h in range(ext.shape[0]):
                row = jnp.broadcast_to(ext[h:h + 1, :], (8, 128))
                val = jnp.where(hi == h, jnp.take_along_axis(row, lo, axis=1, mode='promise_in_bounds'), val)
            fld = jnp.zeros((8, 128), I32)
            for f in range(1, FIELDS):
                fld = fld + jnp.where(val >= f * width, 1, 0)
            idx[0, r0:r0 + 8, c0:c0 + 128] = val - fld * width
            idx[1, r0:r0 + 8, c0:c0 + 128] = lax.shift_left(jnp.ones((8, 128), I32), fld * FIELD_BITS)
    first = lanes_of(ext[0:targets // 128, :])
    nf[:, 0:targets] = jnp.where(iota((nf.shape[0], targets), 0) == first, 1.0, 0.0).astype(BF16)

    block = 16

    def count_block(b, carry):
        base = pl.multiple_of(b * block, block)
        for c0 in range(0, targets, 256):
            row = iota((block, 256), 0) + base
            tot = jnp.zeros((block, 256), I32)
            for k in range(fan_one):
                tot = tot + jnp.where(row == idx[0, k:k + 1, c0:c0 + 256], idx[1, k:k + 1, c0:c0 + 256], 0)
            acc[pl.ds(base, block), c0:c0 + 256] = tot
        return carry

    lax.fori_loop(0, width // block, count_block, 0)
    for f in range(FIELDS):
        cnt = lax.bitwise_and(lax.shift_right_logical(acc[...], f * FIELD_BITS), (1 << FIELD_BITS) - 1)
        nf[f * width:(f + 1) * width, targets:2 * targets] = cnt.astype(F32).astype(BF16)

    for cp in loads[3:]:
        cp.wait()
    small[...] = jnp.full(small.shape, -1, I32)
    small[0:fan_two, 0:seeds] = n2_ref[...]
    small[12:13, 0:seeds] = lab_ref[...]
    m2 = jnp.zeros((targets, 128), F32)
    for k in range(fan_two):
        m2 = m2 + jnp.where(iota((targets, 128), 0) == small[k:k + 1, :], 1.0, 0.0)
    m2 = m2.astype(BF16)
    for src, dst in ((ws1_ref, ws1_t), (wn1_ref, wn1_t), (ws2_ref, ws2_t), (wn2_ref, wn2_t)):
        dst[...] = src[...].T

    pl.when(first_of_plane)(ask_neighbours)

    for cp in asks:
        cp.wait_recv()
    lane = iota((1, 128), 1)
    want = jnp.where(lane < HALO, ask_in[0, 0:1, :], ask_in[1, 0:1, :])
    pick = jnp.where(iota((store, 128), 0) == want, 1.0, 0.0).astype(BF16)
    loads[2].wait()
    out = dot(x_ref[...], pick)
    top = out[0:hrows]
    bot = jnp.concatenate([out[hrows:feat], jnp.zeros((2 * hrows - feat, 128), F32)], axis=0)
    low = iota((hrows, 128), 1) < HALO
    rep[0] = jnp.where(low, top, pltpu.roll(bot, HALO, 1)).astype(BF16)
    rep[1] = jnp.where(low, pltpu.roll(top, HALO, 1), bot).astype(BF16)
    reps = []
    for i, nb in enumerate((right, left)):
        reps.append(pltpu.make_async_remote_copy(rep.at[i], rep_in.at[i], hsend.at[2 + i], hrecv.at[2 + i], device_id=(nb,), device_id_type=MESH))
        reps[-1].start()

    both[...] = dot(x_ref[...], nf[0:store, :])

    for cp in reps:
        cp.wait_recv()
    from_l, from_r = rep_in[0].astype(F32), rep_in[1].astype(F32)
    halo = jnp.concatenate([jnp.where(low, from_l, pltpu.roll(from_r, HALO, 1)).astype(BF16),
                            jnp.where(low, pltpu.roll(from_l, HALO, 1), from_r).astype(BF16)], axis=0)
    rows = both[...] + dot(halo[0:feat], nf[store:store + 2 * HALO, :])
    x_t = rows[:, 0:targets].astype(BF16)
    a_t = (rows[:, targets:] * (1.0 / fan_one)).astype(BF16)
    z = dot(ws1_t[...], x_t) + dot(wn1_t[...], a_t)
    z_ref[...] = z
    h = jnp.maximum(z, 0.0).astype(BF16)
    a2 = (dot(h, m2) * (1.0 / fan_two)).astype(BF16)
    hs = h[:, 0:128]
    ws2, wn2 = ws2_ref[...], wn2_ref[...]
    logits = dot(ws2, hs) + dot(wn2, a2)
    shifted = logits - jnp.max(logits, axis=0, keepdims=True)
    log_prob = shifted - jnp.log(jnp.sum(jnp.exp(shifted), axis=0, keepdims=True))
    hit = iota(logits.shape, 0) == small[12:13, :]
    loss = -jnp.sum(jnp.where(hit, log_prob, 0.0))
    gl = (jnp.exp(log_prob) - jnp.where(hit, 1.0, 0.0)) * scale
    gpad[...] = jnp.zeros(gpad.shape, F32)
    gpad[0:classes, :] = jnp.where(lane < seeds, gl, 0.0)
    gb = gpad[...].astype(BF16)
    d_s2 = dot(gb, hs, 1, 1)
    d_n2 = dot(gb, a2, 1, 1)
    d_s2 = jnp.where(iota(d_s2.shape, 0) == classes, loss, d_s2)
    gc = gb[0:classes]
    g_seed = dot(ws2_t[...], gc)
    g_agg = dot(wn2_t[...], gc) * (1.0 / fan_two)
    p0 = g_agg.astype(BF16)
    r1 = g_agg - p0.astype(F32)
    p1 = r1.astype(BF16)
    p2 = (r1 - p1.astype(F32)).astype(BF16)
    d_h = dot(p0, m2, 1, 1) + (dot(p1, m2, 1, 1) + dot(p2, m2, 1, 1))
    d_h = d_h + jnp.concatenate([g_seed, jnp.zeros((g_seed.shape[0], targets - 128), F32)], axis=1)
    d_z = jnp.where(z_ref[...] > 0, d_h, 0.0).astype(BF16)
    tail = jnp.zeros((2 * hrows - feat, d_z.shape[0]), F32)
    at = 0
    for mat in (jnp.concatenate([dot(x_t, d_z, 1, 1), tail], axis=0),
                jnp.concatenate([dot(a_t, d_z, 1, 1), tail], axis=0), d_s2, d_n2):
        n = mat.shape[0] // 8
        for c0 in range(0, mat.shape[1], 128):
            g[at:at + n] = mat[:, c0:c0 + 128].reshape(n, 8, 128)
            at += n
    if at < g.shape[0]:
        g[at:] = jnp.zeros((g.shape[0] - at, 8, 128), F32)

    copies = []

    def put(src, dst, to):
        k = len(copies)
        cp = pltpu.make_async_remote_copy(src, dst, send.at[k], recv.at[k], device_id=(to,), device_id_type=MESH)
        cp.start()
        copies.append(cp)
        return cp

    other, mine = (1 - core) * half, core * half
    part_a = (nx, xs, xdev, cx, 0, ny, ys, ydev, ca, l1a, w2a, l2a)
    part_b = (ny, ys, ydev, cy, off_b, nx, xs, xdev, cb, l1b, w2b, l2b)
    parts = (part_a, part_b)
    pieces = []
    for i in range(max(nx, ny)):
        for w, p in enumerate(parts):
            if i < p[0]:
                d = (i + 1) % p[0]
                pieces.append((w, d, p[4] + p[1][d] * p[3]))
    arrive = [put(g.at[pl.ds(other + o, parts[w][3])], rc.at[pl.ds(o, parts[w][3])], mate) for w, d, o in pieces]
    first_in = [{}, {}]
    for (w, d, o), cp in zip(pieces, arrive):
        _, _, to, n, _, n2, sub, _, c, land, _, _ = parts[w]
        cp.wait_recv()
        part[pl.ds(o, n)] = g[pl.ds(mine + o, n)] + rc[pl.ds(o, n)]
        if d:
            for i in range(n2):
                e = (i + 1) % n2
                first_in[w][d, e] = put(part.at[pl.ds(o + sub[e] * c, c)], land.at[d - 1, e], to[d])
    second_in, sums = [[], []], [None, None]
    for i in range(max(nx, ny)):
        for w, (n1, own, _, n, off, n2, sub, to, c, land, w2, l2) in enumerate(parts):
            if i < n2:
                e = (i + 1) % n2
                tot = part[pl.ds(off + own[0] * n + sub[e] * c, c)]
                for d in range(1, n1):
                    first_in[w][d, e].wait_recv()
                    tot = tot + land[d - 1, e]
                if e:
                    w2[e - 1] = tot
                    second_in[w].append(put(w2.at[e - 1], l2.at[e - 1], to[e]))
                else:
                    sums[w] = tot
    for w, at, n in ((0, 0, ca), (1, ca, cb)):
        tot = sums[w]
        for e, cp in enumerate(second_in[w]):
            cp.wait_recv()
            tot = tot + parts[w][11][e]
        zc[at:at + n] = tot
    for d in range(1, nz):
        pl.when(mz + d < nz)(functools.partial(pl.semaphore_wait, up.at[d], 1))
    quarter = lax.rem(mz, nq)
    in_z = [put(zc.at[pl.ds((zn * lax.rem(zs[d], nq)) // nq, zsize)], lz.at[mz], zdev[d]) for d in range(1, nz)]
    lz[mz] = zc[pl.ds((zn * quarter) // nq, zsize)]
    for cp in in_z:
        cp.wait_recv()
    tot = lz[0]
    for z in range(1, nz):
        tot = tot + lz[z]
    zg[quarter] = tot
    done = 0
    if nq == 4:
        far = lax.rem(mz + 2 + 4 * lax.rem(mz, 2), nz)
        targets_z = (zdev[1], zdev[nz - 1], dev(far, my, mx, core))
        done = list(copies) + asks + reps
        in_z = [put(zg.at[quarter], zg.at[quarter], to) for to in targets_z]
        for cp in done:
            cp.wait_send()
        done = len(copies) - 3
        for cp in in_z:
            cp.wait_recv()
    base = [mine + p[4] + p[1][0] * p[3] for p in parts]
    spots = [base[w] + p[6][0] * p[8] for w, p in enumerate(parts)]
    for q in range(nq):
        lo = (zn * q) // nq
        end = (zn * (q + 1)) // nq
        for t in range(lo, end):
            at = spots[0] + t if t < ca else spots[1] + (t - ca)
            r_ref[pl.ds(at, 1)] = zg[q, t - lo:t - lo + 1]
    back = []

    def spread(w, at):
        n1, _, to, _, _, _, _, _, c, _, _, _ = parts[w]
        got = [put(r_ref.at[pl.ds(at, c)], r_ref.at[pl.ds(at, c)], to[d]) for d in range(1, n1)]
        back.append(put(r_ref.at[pl.ds(at, c)], r_ref.at[pl.ds(at, c)], mate))
        return got

    second_in = [[], []]
    for w, p in enumerate(parts):
        for e in range(1, p[5]):
            second_in[w].append(put(r_ref.at[pl.ds(spots[w], p[8])], r_ref.at[pl.ds(spots[w], p[8])], p[7][e]))
    first_in = [[spread(w, spots[w])] for w in range(2)]
    for i in range(max(nx, ny)):
        for w, (n1, own, _, n, off, n2, sub, _, c, _, _, _) in enumerate(parts):
            if i < n2 - 1:
                second_in[w][i].wait_recv()
                first_in[w].append(spread(w, base[w] + sub[n2 - 1 - i] * c))
    for cp in copies[done:] + ([] if done else asks + reps):
        cp.wait_send()
    sent = len(copies)
    for i in range(max(nx, ny)):
        for w, (n1, own, _, n, off, n2, sub, _, c, _, _, _) in enumerate(parts):
            if i < n2:
                for d in range(1, n1):
                    first_in[w][i][d - 1].wait_recv()
                    at = mine + off + own[n1 - d] * n + sub[(n2 - i) % n2] * c
                    back.append(put(r_ref.at[pl.ds(at, c)], r_ref.at[pl.ds(at, c)], mate))
    for cp in back:
        cp.wait_recv()
    for cp in copies[sent:]:
        cp.wait_send()


def copy_count(group):
    nx, ny, nz = dims_of(group)
    return nx + ny + 2 * ((nx - 1) * ny + (ny - 1) * nx + nx - 1 + ny - 1) + nz - 1 + (3 if nz == 8 else 0) + 2 * nx * ny


def output_kernel(scale, r_ref, loss_ref, s1_hbm, n1_hbm, s2_hbm, n2_hbm, s1, n1, s2, n2, sem):
    at, k = 0, 0
    classes = s2.shape[0]
    copies = []
    for ref, hbm in ((s1, s1_hbm), (n1, n1_hbm), (s2, s2_hbm), (n2, n2_hbm)):
        rows, cols = ref.shape
        n = -(-rows // 8)
        step = n if n < 16 else 19
        for r0 in range(0, n, step):
            lo, hi = r0 * 8, min(rows, (r0 + step) * 8)
            for c in range(cols // 128):
                val = r_ref[at + c * n + r0:at + c * n + r0 + step].reshape(step * 8, 128)
                ref[lo:hi, c * 128:(c + 1) * 128] = val[0:hi - lo]
                if ref is s2 and c == 0:
                    loss_ref[...] = val[classes:classes + 1, 0:1] * scale
            cp = pltpu.make_async_copy(ref.at[lo:hi], hbm.at[lo:hi], sem.at[k])
            cp.start()
            copies.append(cp)
            k += 1
        at += n * (cols // 128)
    for cp in copies:
        cp.wait()


def solution(mesh):
    group = mesh.shape['g']

    def device_step(x_local, front_ids, nbr_one, nbr_two, labels, w_self1, w_nbr1, w_self2, w_nbr2):
        store, feat = x_local.shape
        targets, fan_one = nbr_one.shape
        seeds, fan_two = nbr_two.shape
        hidden, classes = w_self2.shape
        frows = -(-feat // 32) * 32
        scale = 1.0 / (group * seeds)
        fid = front_ids.reshape(-1, 128)
        width = -(-(store + 2 * HALO) // (FIELDS * 16)) * 16
        nx, ny, nz = dims_of(group)
        ca, cb = chunks_of(group)
        cx, cy, zn = ny * ca, nx * cb, ca + cb
        nq = max(1, nz // 2)
        zsize = -(-zn // nq)
        half = nx * cx + ny * cy
        total = 2 * half
        n = copy_count(group)
        dma = pltpu.SemaphoreType.DMA

        def buf(*lead):
            return VMEM((*lead, 8, 128), F32)

        vm, hbm = pl.BlockSpec(memory_space=VMEM), pl.BlockSpec(memory_space=pl.ANY)
        sums = pl.pallas_call(
            functools.partial(step_kernel, group, scale),
            name='train_step',
            out_shape=VMEM((total, 8, 128), F32),
            in_specs=[hbm] * 9,
            out_specs=vm,
            scratch_shapes=[
                VMEM(fid.shape, I32), VMEM((feat, store), BF16), VMEM((fan_one, targets), I32), VMEM((fan_two, seeds), I32),
                VMEM((1, seeds), I32), VMEM((feat, hidden), BF16), VMEM((feat, hidden), BF16), VMEM((classes, hidden), BF16),
                VMEM((classes, hidden), BF16), dma((9,)),
                VMEM((hidden, feat), BF16), VMEM((hidden, feat), BF16), VMEM((hidden, classes), BF16), VMEM((hidden, classes), BF16),
                VMEM((8, 128), I32), VMEM((2, 8, 128), I32), VMEM((2, frows // 2, 128), BF16),
                VMEM((2, frows // 2, 128), BF16), dma((4,)), dma((4,)),
                pltpu.SemaphoreType.REGULAR((nz,)),
                VMEM((16, 128), I32), VMEM((2, -(-fan_one // 8) * 8, targets), I32), VMEM((width, targets), I32),
                VMEM((FIELDS * width, 2 * targets), BF16), VMEM((feat, 2 * targets), F32), VMEM((hidden, targets), F32),
                VMEM((-(-classes // 16) * 16, 128), F32), buf(total),
                buf(half), buf(half), buf(nx - 1, ny, ca), buf(ny - 1, nx, cb), buf(ny - 1, ca), buf(nx - 1, cb),
                buf(ny - 1, ca), buf(nx - 1, cb), buf(zn), buf(nz, zsize), buf(nq, zsize),
                dma((n,)), dma((n,))],
            compiler_params=pltpu.CompilerParams(collective_id=0, has_side_effects=True,
                                                 vmem_limit_bytes=60 * 1024 * 1024),
        )(fid, x_local.T, nbr_one.T, nbr_two.T, labels.reshape(1, -1), w_self1, w_nbr1, w_self2.T, w_nbr2.T)
        loss, d_s1, d_n1, d_s2, d_n2 = pl.pallas_call(
            functools.partial(output_kernel, scale),
            name='split_outputs',
            out_shape=[jax.ShapeDtypeStruct((1, 1), F32), jax.ShapeDtypeStruct((feat, hidden), F32),
                       jax.ShapeDtypeStruct((feat, hidden), F32), jax.ShapeDtypeStruct((classes, hidden), F32),
                       jax.ShapeDtypeStruct((classes, hidden), F32)],
            in_specs=[vm], out_specs=[vm] + [hbm] * 4,
            scratch_shapes=[VMEM((feat, hidden), F32), VMEM((feat, hidden), F32), VMEM((classes, hidden), F32),
                            VMEM((classes, hidden), F32), dma((10,))],
        )(pltpu.with_memory_space_constraint(sums, VMEM))
        return loss[0, 0], d_s1, d_n1, d_s2.T, d_n2.T

    return jax.shard_map(device_step, mesh=mesh,
                         in_specs=(P('g', None), P('g'), P('g', None), P('g', None), P('g'), P(), P(), P(), P()),
                         out_specs=(P(), P(), P(), P(), P()), check_vma=False)
```

```python
import functools

import jax
import jax.numpy as jnp
from jax import lax
from jax.experimental import pallas as pl
from jax.experimental.pallas import tpu as pltpu
from jax.sharding import PartitionSpec as P

MESH = pl.DeviceIdType.MESH
F32, BF16, I32 = jnp.float32, jnp.bfloat16, jnp.int32
VMEM = pltpu.VMEM

HALO = 64
FIELDS, FIELD_BITS = 6, 5


def dims_of(group):
    return {256: (4, 4, 8), 16: (2, 2, 2)}[group]


def chunks_of(group):
    return {256: (6, 5), 16: (21, 20)}[group]


def dot(a, b, ca=1, cb=0):
    return lax.dot_general(a, b, (((ca,), (cb,)), ((), ())), preferred_element_type=F32)


def iota(shape, dim):
    return lax.broadcasted_iota(I32, shape, dim)


def far_first(n):
    return sorted(range(1, n), key=lambda d: -min(d, n - d)) + [0]


def frontier_ext(fid, me, group, rows_log2):
    store = 1 << rows_log2
    owner = lax.shift_right_logical(fid, rows_log2)
    off = lax.bitwise_and(fid, store - 1)
    left, right = lax.rem(me + group - 1, group), lax.rem(me + 1, group)
    is_l, is_r = owner == left, owner == right
    mask = jnp.concatenate([jnp.where(is_l, 1.0, 0.0), jnp.where(is_r, 1.0, 0.0)], axis=0).astype(BF16)
    n = fid.shape[0]
    upper = jnp.where(iota((128, 128), 0) < iota((128, 128), 1), 1.0, 0.0).astype(BF16)
    ri, ci = iota((2 * n, 2 * n), 0), iota((2 * n, 2 * n), 1)
    before = jnp.where((ci < ri) & ((ci < n) == (ri < n)), 1.0, 0.0).astype(BF16)
    ones = jnp.ones((128, 128), BF16)
    rank = dot(mask, upper) + dot(dot(before, mask).astype(BF16), ones)
    rank = rank.astype(I32)
    rank_l, rank_r = rank[:n], rank[n:]
    ext = jnp.where(is_l, store + rank_l, jnp.where(is_r, store + HALO + rank_r, off))
    return ext, off


def lanes_of(a):
    return jnp.concatenate([a[i:i + 1, :] for i in range(a.shape[0])], axis=1)


def ask_rows(ext, off, store):
    key = lanes_of(ext) - store
    offs = lanes_of(off)
    pick = jnp.where(iota((2 * HALO, key.shape[1]), 0) == key, 1.0, 0.0).astype(BF16)
    row = iota((16, key.shape[1]), 0)
    hi, lo = lax.shift_right_logical(offs, 6), lax.bitwise_and(offs, 63)
    parts = jnp.where(row == 0, hi, jnp.where(row == 1, lo, 0)).astype(F32).astype(BF16)
    got = dot(parts, pick, 1, 1).astype(I32)
    return got[0:1] * 64 + got[1:2]


def step_kernel(group, scale, fid_hbm, x_hbm, n1_hbm, n2_hbm, lab_hbm, ws1_hbm, wn1_hbm, ws2_hbm, wn2_hbm, r_ref,
                fid_ref, x_ref, n1_ref, n2_ref, lab_ref, ws1_ref, wn1_ref, ws2_ref, wn2_ref, in_sem,
                ws1_t, wn1_t, ws2_t, wn2_t, ask, ask_in, rep, rep_in, hsend, hrecv, up,
                small, idx, acc, nf, both, z_ref, gpad, g,
                rc, part, l1a, l1b, w2a, w2b, l2a, l2b, zc, lz, zg, send, recv):
    nx, ny, nz = dims_of(group)
    ca, cb = chunks_of(group)
    cx, cy, zn = ny * ca, nx * cb, ca + cb
    nq = max(1, nz // 2)
    zsize = -(-zn // nq)
    off_b = nx * cx
    half = off_b + ny * cy
    me = lax.axis_index('g')
    core = lax.rem(me, 2)
    mx = lax.rem(me // 2, nx)
    my = lax.rem(me // (2 * nx), ny)
    mz = me // (2 * nx * ny)

    def dev(z, y, x, c):
        return ((z * ny + y) * nx + x) * 2 + c

    mate = dev(mz, my, mx, 1 - core)
    xs = [lax.rem(mx + d, nx) for d in range(nx)]
    ys = [lax.rem(my + d, ny) for d in range(ny)]
    zs = [lax.rem(mz + d, nz) for d in range(nz)]
    xdev = [dev(mz, my, x, core) for x in xs]
    ydev = [dev(mz, y, mx, core) for y in ys]
    zdev = [dev(z, my, mx, core) for z in zs]
    left, right = lax.rem(me + group - 1, group), lax.rem(me + 1, group)

    barrier = pltpu.get_barrier_semaphore()
    peers = [left, right, mate] + xdev[1:] + ydev[1:]

    def signal(sem, to):
        pl.semaphore_signal(sem, inc=1, device_id=(to,), device_id_type=MESH)

    for nb in peers:
        pl.semaphore_signal(barrier, inc=1, device_id=(nb,), device_id_type=MESH)
    for d in range(1, nz):
        pl.when(mz + d < nz)(functools.partial(signal, barrier, zdev[d]))
    loads = [pltpu.make_async_copy(src, dst, in_sem.at[i]) for i, (src, dst) in
             enumerate(((fid_hbm, fid_ref), (n1_hbm, n1_ref), (x_hbm, x_ref), (n2_hbm, n2_ref), (lab_hbm, lab_ref),
                        (ws1_hbm, ws1_ref), (wn1_hbm, wn1_ref), (ws2_hbm, ws2_ref), (wn2_hbm, wn2_ref)))]
    for cp in loads:
        cp.start()

    feat, store = x_ref.shape
    targets = n1_ref.shape[1]
    fan_one = n1_ref.shape[0]
    fan_two, seeds = n2_ref.shape
    classes = ws2_ref.shape[0]
    width = acc.shape[0]
    hrows = rep.shape[1]
    loads[0].wait()
    ext, off = frontier_ext(fid_ref[...], me, group, store.bit_length() - 1)
    ask[...] = jnp.broadcast_to(ask_rows(ext, off, store), ask.shape)
    asks = []
    for i, nb in enumerate((left, right)):
        asks.append(pltpu.make_async_remote_copy(ask, ask_in.at[i], hsend.at[i], hrecv.at[i], device_id=(nb,), device_id_type=MESH))

    def ask_neighbours():
        pl.semaphore_wait(barrier, len(peers) + mz)
        for cp in asks:
            cp.start()
        for d in range(1, nz):
            pl.when(mz + d >= nz)(functools.partial(signal, up.at[nz - d], zdev[d]))

    first_of_plane = lax.rem(me, 2 * nx * ny) == 0
    pl.when(jnp.logical_not(first_of_plane))(ask_neighbours)

    loads[1].wait()
    for r0 in range(0, fan_one, 8):
        nr = min(8, fan_one - r0)
        for c0 in range(0, targets, 128):
            pos = n1_ref[r0:r0 + nr, c0:c0 + 128]
            if nr < 8:
                pos = jnp.broadcast_to(pos[0:1], (8, 128)) if nr == 1 else jnp.concatenate([pos, pos[0:8 - nr]], axis=0)
            hi = lax.shift_right_logical(pos, 7)
            lo = lax.bitwise_and(pos, 127)
            val = jnp.zeros((8, 128), I32)
            for h in range(ext.shape[0]):
                row = jnp.broadcast_to(ext[h:h + 1, :], (8, 128))
                val = jnp.where(hi == h, jnp.take_along_axis(row, lo, axis=1, mode='promise_in_bounds'), val)
            fld = jnp.zeros((8, 128), I32)
            for f in range(1, FIELDS):
                fld = fld + jnp.where(val >= f * width, 1, 0)
            idx[0, r0:r0 + 8, c0:c0 + 128] = val - fld * width
            idx[1, r0:r0 + 8, c0:c0 + 128] = lax.shift_left(jnp.ones((8, 128), I32), fld * FIELD_BITS)
    first = lanes_of(ext[0:targets // 128, :])
    nf[:, 0:targets] = jnp.where(iota((nf.shape[0], targets), 0) == first, 1.0, 0.0).astype(BF16)

    block = 16

    def count_block(b, carry):
        base = pl.multiple_of(b * block, block)
        for c0 in range(0, targets, 256):
            row = iota((block, 256), 0) + base
            tot = jnp.zeros((block, 256), I32)
            for k in range(fan_one):
                tot = tot + jnp.where(row == idx[0, k:k + 1, c0:c0 + 256], idx[1, k:k + 1, c0:c0 + 256], 0)
            acc[pl.ds(base, block), c0:c0 + 256] = tot
        return carry

    lax.fori_loop(0, width // block, count_block, 0)
    for f in range(FIELDS):
        cnt = lax.bitwise_and(lax.shift_right_logical(acc[...], f * FIELD_BITS), (1 << FIELD_BITS) - 1)
        nf[f * width:(f + 1) * width, targets:2 * targets] = cnt.astype(F32).astype(BF16)

    for cp in loads[3:]:
        cp.wait()
    small[...] = jnp.full(small.shape, -1, I32)
    small[0:fan_two, 0:seeds] = n2_ref[...]
    small[12:13, 0:seeds] = lab_ref[...]
    m2 = jnp.zeros((targets, 128), F32)
    for k in range(fan_two):
        m2 = m2 + jnp.where(iota((targets, 128), 0) == small[k:k + 1, :], 1.0, 0.0)
    m2 = m2.astype(BF16)
    for src, dst in ((ws1_ref, ws1_t), (wn1_ref, wn1_t), (ws2_ref, ws2_t), (wn2_ref, wn2_t)):
        dst[...] = src[...].T

    pl.when(first_of_plane)(ask_neighbours)

    for cp in asks:
        cp.wait_recv()
    lane = iota((1, 128), 1)
    want = jnp.where(lane < HALO, ask_in[0, 0:1, :], ask_in[1, 0:1, :])
    pick = jnp.where(iota((store, 128), 0) == want, 1.0, 0.0).astype(BF16)
    loads[2].wait()
    out = dot(x_ref[...], pick)
    top = out[0:hrows]
    bot = jnp.concatenate([out[hrows:feat], jnp.zeros((2 * hrows - feat, 128), F32)], axis=0)
    low = iota((hrows, 128), 1) < HALO
    rep[0] = jnp.where(low, top, pltpu.roll(bot, HALO, 1)).astype(BF16)
    rep[1] = jnp.where(low, pltpu.roll(top, HALO, 1), bot).astype(BF16)
    reps = []
    for i, nb in enumerate((right, left)):
        reps.append(pltpu.make_async_remote_copy(rep.at[i], rep_in.at[i], hsend.at[2 + i], hrecv.at[2 + i], device_id=(nb,), device_id_type=MESH))
        reps[-1].start()

    both[...] = dot(x_ref[...], nf[0:store, :])

    for cp in reps:
        cp.wait_recv()
    from_l, from_r = rep_in[0].astype(F32), rep_in[1].astype(F32)
    halo = jnp.concatenate([jnp.where(low, from_l, pltpu.roll(from_r, HALO, 1)).astype(BF16),
                            jnp.where(low, pltpu.roll(from_l, HALO, 1), from_r).astype(BF16)], axis=0)
    rows = both[...] + dot(halo[0:feat], nf[store:store + 2 * HALO, :])
    x_t = rows[:, 0:targets].astype(BF16)
    a_t = (rows[:, targets:] * (1.0 / fan_one)).astype(BF16)
    z = dot(ws1_t[...], x_t) + dot(wn1_t[...], a_t)
    z_ref[...] = z
    h = jnp.maximum(z, 0.0).astype(BF16)
    a2 = (dot(h, m2) * (1.0 / fan_two)).astype(BF16)
    hs = h[:, 0:128]
    ws2, wn2 = ws2_ref[...], wn2_ref[...]
    logits = dot(ws2, hs) + dot(wn2, a2)
    shifted = logits - jnp.max(logits, axis=0, keepdims=True)
    log_prob = shifted - jnp.log(jnp.sum(jnp.exp(shifted), axis=0, keepdims=True))
    hit = iota(logits.shape, 0) == small[12:13, :]
    loss = -jnp.sum(jnp.where(hit, log_prob, 0.0))
    gl = (jnp.exp(log_prob) - jnp.where(hit, 1.0, 0.0)) * scale
    gpad[...] = jnp.zeros(gpad.shape, F32)
    gpad[0:classes, :] = jnp.where(lane < seeds, gl, 0.0)
    gb = gpad[...].astype(BF16)
    d_s2 = dot(gb, hs, 1, 1)
    d_n2 = dot(gb, a2, 1, 1)
    d_s2 = jnp.where(iota(d_s2.shape, 0) == classes, loss, d_s2)
    gc = gb[0:classes]
    g_seed = dot(ws2_t[...], gc)
    g_agg = dot(wn2_t[...], gc) * (1.0 / fan_two)
    p0 = g_agg.astype(BF16)
    r1 = g_agg - p0.astype(F32)
    p1 = r1.astype(BF16)
    p2 = (r1 - p1.astype(F32)).astype(BF16)
    d_h = dot(p0, m2, 1, 1) + (dot(p1, m2, 1, 1) + dot(p2, m2, 1, 1))
    d_h = d_h + jnp.concatenate([g_seed, jnp.zeros((g_seed.shape[0], targets - 128), F32)], axis=1)
    d_z = jnp.where(z_ref[...] > 0, d_h, 0.0).astype(BF16)
    tail = jnp.zeros((2 * hrows - feat, d_z.shape[0]), F32)
    at = 0
    for mat in (jnp.concatenate([dot(x_t, d_z, 1, 1), tail], axis=0),
                jnp.concatenate([dot(a_t, d_z, 1, 1), tail], axis=0), d_s2, d_n2):
        n = mat.shape[0] // 8
        for c0 in range(0, mat.shape[1], 128):
            g[at:at + n] = mat[:, c0:c0 + 128].reshape(n, 8, 128)
            at += n
    if at < g.shape[0]:
        g[at:] = jnp.zeros((g.shape[0] - at, 8, 128), F32)

    copies = []

    def put(src, dst, to):
        k = len(copies)
        cp = pltpu.make_async_remote_copy(src, dst, send.at[k], recv.at[k], device_id=(to,), device_id_type=MESH)
        cp.start()
        copies.append(cp)
        return cp

    other, mine = (1 - core) * half, core * half
    part_a = (nx, xs, xdev, cx, 0, ny, ys, ydev, ca, l1a, w2a, l2a)
    part_b = (ny, ys, ydev, cy, off_b, nx, xs, xdev, cb, l1b, w2b, l2b)
    parts = (part_a, part_b)
    pieces = []
    for i in range(max(nx, ny)):
        for w, p in enumerate(parts):
            if i < p[0]:
                d = far_first(p[0])[i]
                pieces.append((w, d, p[4] + p[1][d] * p[3]))
    arrive = [put(g.at[pl.ds(other + o, parts[w][3])], rc.at[pl.ds(o, parts[w][3])], mate) for w, d, o in pieces]
    first_in = [{}, {}]
    for (w, d, o), cp in zip(pieces, arrive):
        _, _, to, n, _, n2, sub, _, c, land, _, _ = parts[w]
        cp.wait_recv()
        part[pl.ds(o, n)] = g[pl.ds(mine + o, n)] + rc[pl.ds(o, n)]
        if d:
            for i in range(n2):
                e = far_first(n2)[i]
                first_in[w][d, e] = put(part.at[pl.ds(o + sub[e] * c, c)], land.at[d - 1, e], to[d])
    second_in, sums = [[], []], [None, None]
    for i in range(max(nx, ny)):
        for w, (n1, own, _, n, off, n2, sub, to, c, land, w2, l2) in enumerate(parts):
            if i < n2:
                e = far_first(n2)[i]
                tot = part[pl.ds(off + own[0] * n + sub[e] * c, c)]
                for d in range(1, n1):
                    first_in[w][d, e].wait_recv()
                    tot = tot + land[d - 1, e]
                if e:
                    w2[e - 1] = tot
                    second_in[w].append((e, put(w2.at[e - 1], l2.at[e - 1], to[e])))
                else:
                    sums[w] = tot
    for w, at, n in ((0, 0, ca), (1, ca, cb)):
        tot = sums[w]
        for e, cp in second_in[w]:
            cp.wait_recv()
            tot = tot + parts[w][11][e - 1]
        zc[at:at + n] = tot
    for d in range(1, nz):
        pl.when(mz + d < nz)(functools.partial(pl.semaphore_wait, up.at[d], 1))
    quarter = lax.rem(mz, nq)
    in_z = [put(zc.at[pl.ds((zn * lax.rem(zs[d], nq)) // nq, zsize)], lz.at[mz], zdev[d]) for d in far_first(nz)[:-1]]
    lz[mz] = zc[pl.ds((zn * quarter) // nq, zsize)]
    for cp in in_z:
        cp.wait_recv()
    tot = lz[0]
    for z in range(1, nz):
        tot = tot + lz[z]
    zg[quarter] = tot
    done = 0
    if nq == 4:
        far = lax.rem(mz + 2 + 4 * lax.rem(mz, 2), nz)
        targets_z = (dev(far, my, mx, core), zdev[1], zdev[nz - 1])
        done = list(copies) + asks + reps
        in_z = [put(zg.at[quarter], zg.at[quarter], to) for to in targets_z]
        for cp in done:
            cp.wait_send()
        done = len(copies) - 3
        for cp in in_z:
            cp.wait_recv()
    base = [mine + p[4] + p[1][0] * p[3] for p in parts]
    spots = [base[w] + p[6][0] * p[8] for w, p in enumerate(parts)]
    for q in range(nq):
        lo = (zn * q) // nq
        end = (zn * (q + 1)) // nq
        for t in range(lo, end):
            at = spots[0] + t if t < ca else spots[1] + (t - ca)
            r_ref[pl.ds(at, 1)] = zg[q, t - lo:t - lo + 1]
    back = []

    def spread(w, at):
        n1, _, to, _, _, _, _, _, c, _, _, _ = parts[w]
        got = {d: put(r_ref.at[pl.ds(at, c)], r_ref.at[pl.ds(at, c)], to[d]) for d in far_first(n1)[:-1]}
        back.append(put(r_ref.at[pl.ds(at, c)], r_ref.at[pl.ds(at, c)], mate))
        return got

    second_in = [{}, {}]
    for w, p in enumerate(parts):
        for e in far_first(p[5])[:-1]:
            second_in[w][e] = (put(r_ref.at[pl.ds(spots[w], p[8])], r_ref.at[pl.ds(spots[w], p[8])], p[7][e]))
    first_in = [[spread(w, spots[w])] for w in range(2)]
    for i in range(max(nx, ny)):
        for w, (n1, own, _, n, off, n2, sub, _, c, _, _, _) in enumerate(parts):
            if i < n2 - 1:
                e = far_first(n2)[n2 - 2 - i]
                second_in[w][e].wait_recv()
                first_in[w].append(spread(w, base[w] + sub[n2 - e] * c))
    for cp in copies[done:] + ([] if done else asks + reps):
        cp.wait_send()
    sent = len(copies)
    for i in range(max(nx, ny)):
        for w, (n1, own, _, n, off, n2, sub, _, c, _, _, _) in enumerate(parts):
            if i < n2:
                e = far_first(n2)[n2 - 1 - i]
                for d in reversed(far_first(n1)[:-1]):
                    first_in[w][i][d].wait_recv()
                    at = mine + off + own[n1 - d] * n + sub[(n2 - e) % n2] * c
                    back.append(put(r_ref.at[pl.ds(at, c)], r_ref.at[pl.ds(at, c)], mate))
    for cp in back:
        cp.wait_recv()
    for cp in copies[sent:]:
        cp.wait_send()


def copy_count(group):
    nx, ny, nz = dims_of(group)
    return nx + ny + 2 * ((nx - 1) * ny + (ny - 1) * nx + nx - 1 + ny - 1) + nz - 1 + (3 if nz == 8 else 0) + 2 * nx * ny


def output_kernel(scale, r_ref, loss_ref, s1_hbm, n1_hbm, s2_hbm, n2_hbm, s1, n1, s2, n2, sem):
    at, k = 0, 0
    classes = s2.shape[0]
    copies = []
    for ref, hbm in ((s1, s1_hbm), (n1, n1_hbm), (s2, s2_hbm), (n2, n2_hbm)):
        rows, cols = ref.shape
        n = -(-rows // 8)
        step = n if n < 16 else 19
        for r0 in range(0, n, step):
            lo, hi = r0 * 8, min(rows, (r0 + step) * 8)
            for c in range(cols // 128):
                val = r_ref[at + c * n + r0:at + c * n + r0 + step].reshape(step * 8, 128)
                ref[lo:hi, c * 128:(c + 1) * 128] = val[0:hi - lo]
                if ref is s2 and c == 0:
                    loss_ref[...] = val[classes:classes + 1, 0:1] * scale
            cp = pltpu.make_async_copy(ref.at[lo:hi], hbm.at[lo:hi], sem.at[k])
            cp.start()
            copies.append(cp)
            k += 1
        at += n * (cols // 128)
    for cp in copies:
        cp.wait()


def solution(mesh):
    group = mesh.shape['g']

    def device_step(x_local, front_ids, nbr_one, nbr_two, labels, w_self1, w_nbr1, w_self2, w_nbr2):
        store, feat = x_local.shape
        targets, fan_one = nbr_one.shape
        seeds, fan_two = nbr_two.shape
        hidden, classes = w_self2.shape
        frows = -(-feat // 32) * 32
        scale = 1.0 / (group * seeds)
        fid = front_ids.reshape(-1, 128)
        width = -(-(store + 2 * HALO) // (FIELDS * 16)) * 16
        nx, ny, nz = dims_of(group)
        ca, cb = chunks_of(group)
        cx, cy, zn = ny * ca, nx * cb, ca + cb
        nq = max(1, nz // 2)
        zsize = -(-zn // nq)
        half = nx * cx + ny * cy
        total = 2 * half
        n = copy_count(group)
        dma = pltpu.SemaphoreType.DMA

        def buf(*lead):
            return VMEM((*lead, 8, 128), F32)

        vm, hbm = pl.BlockSpec(memory_space=VMEM), pl.BlockSpec(memory_space=pl.ANY)
        sums = pl.pallas_call(
            functools.partial(step_kernel, group, scale),
            name='train_step',
            out_shape=VMEM((total, 8, 128), F32),
            in_specs=[hbm] * 9,
            out_specs=vm,
            scratch_shapes=[
                VMEM(fid.shape, I32), VMEM((feat, store), BF16), VMEM((fan_one, targets), I32), VMEM((fan_two, seeds), I32),
                VMEM((1, seeds), I32), VMEM((feat, hidden), BF16), VMEM((feat, hidden), BF16), VMEM((classes, hidden), BF16),
                VMEM((classes, hidden), BF16), dma((9,)),
                VMEM((hidden, feat), BF16), VMEM((hidden, feat), BF16), VMEM((hidden, classes), BF16), VMEM((hidden, classes), BF16),
                VMEM((8, 128), I32), VMEM((2, 8, 128), I32), VMEM((2, frows // 2, 128), BF16),
                VMEM((2, frows // 2, 128), BF16), dma((4,)), dma((4,)),
                pltpu.SemaphoreType.REGULAR((nz,)),
                VMEM((16, 128), I32), VMEM((2, -(-fan_one // 8) * 8, targets), I32), VMEM((width, targets), I32),
                VMEM((FIELDS * width, 2 * targets), BF16), VMEM((feat, 2 * targets), F32), VMEM((hidden, targets), F32),
                VMEM((-(-classes // 16) * 16, 128), F32), buf(total),
                buf(half), buf(half), buf(nx - 1, ny, ca), buf(ny - 1, nx, cb), buf(ny - 1, ca), buf(nx - 1, cb),
                buf(ny - 1, ca), buf(nx - 1, cb), buf(zn), buf(nz, zsize), buf(nq, zsize),
                dma((n,)), dma((n,))],
            compiler_params=pltpu.CompilerParams(collective_id=0, has_side_effects=True,
                                                 vmem_limit_bytes=60 * 1024 * 1024),
        )(fid, x_local.T, nbr_one.T, nbr_two.T, labels.reshape(1, -1), w_self1, w_nbr1, w_self2.T, w_nbr2.T)
        loss, d_s1, d_n1, d_s2, d_n2 = pl.pallas_call(
            functools.partial(output_kernel, scale),
            name='split_outputs',
            out_shape=[jax.ShapeDtypeStruct((1, 1), F32), jax.ShapeDtypeStruct((feat, hidden), F32),
                       jax.ShapeDtypeStruct((feat, hidden), F32), jax.ShapeDtypeStruct((classes, hidden), F32),
                       jax.ShapeDtypeStruct((classes, hidden), F32)],
            in_specs=[vm], out_specs=[vm] + [hbm] * 4,
            scratch_shapes=[VMEM((feat, hidden), F32), VMEM((feat, hidden), F32), VMEM((classes, hidden), F32),
                            VMEM((classes, hidden), F32), dma((10,))],
        )(pltpu.with_memory_space_constraint(sums, VMEM))
        return loss[0, 0], d_s1, d_n1, d_s2.T, d_n2.T

    return jax.shard_map(device_step, mesh=mesh,
                         in_specs=(P('g', None), P('g'), P('g', None), P('g', None), P('g'), P(), P(), P(), P()),
                         out_specs=(P(), P(), P(), P(), P()), check_vma=False)
```

```python
import functools

import jax
import jax.numpy as jnp
from jax import lax
from jax.experimental import pallas as pl
from jax.experimental.pallas import tpu as pltpu
from jax.sharding import PartitionSpec as P

MESH = pl.DeviceIdType.MESH
F32, BF16, I32 = jnp.float32, jnp.bfloat16, jnp.int32
VMEM = pltpu.VMEM

HALO = 64
FIELDS, FIELD_BITS = 6, 5


def dims_of(group):
    return {256: (4, 4, 8), 16: (2, 2, 2)}[group]


def chunks_of(group):
    return {256: (6, 5), 16: (21, 20)}[group]


def dot(a, b, ca=1, cb=0):
    return lax.dot_general(a, b, (((ca,), (cb,)), ((), ())), preferred_element_type=F32)


def iota(shape, dim):
    return lax.broadcasted_iota(I32, shape, dim)


def far_first(n):
    return sorted(range(1, n), key=lambda d: -min(d, n - d)) + [0]


def frontier_ext(fid, me, group, rows_log2):
    store = 1 << rows_log2
    owner = lax.shift_right_logical(fid, rows_log2)
    off = lax.bitwise_and(fid, store - 1)
    left, right = lax.rem(me + group - 1, group), lax.rem(me + 1, group)
    is_l, is_r = owner == left, owner == right
    mask = jnp.concatenate([jnp.where(is_l, 1.0, 0.0), jnp.where(is_r, 1.0, 0.0)], axis=0).astype(BF16)
    n = fid.shape[0]
    upper = jnp.where(iota((128, 128), 0) < iota((128, 128), 1), 1.0, 0.0).astype(BF16)
    ri, ci = iota((2 * n, 2 * n), 0), iota((2 * n, 2 * n), 1)
    before = jnp.where((ci < ri) & ((ci < n) == (ri < n)), 1.0, 0.0).astype(BF16)
    ones = jnp.ones((128, 128), BF16)
    rank = dot(mask, upper) + dot(dot(before, mask).astype(BF16), ones)
    rank = rank.astype(I32)
    rank_l, rank_r = rank[:n], rank[n:]
    ext = jnp.where(is_l, store + rank_l, jnp.where(is_r, store + HALO + rank_r, off))
    return ext, off


def lanes_of(a):
    return jnp.concatenate([a[i:i + 1, :] for i in range(a.shape[0])], axis=1)


def ask_rows(ext, off, store):
    key = lanes_of(ext) - store
    offs = lanes_of(off)
    pick = jnp.where(iota((2 * HALO, key.shape[1]), 0) == key, 1.0, 0.0).astype(BF16)
    row = iota((16, key.shape[1]), 0)
    hi, lo = lax.shift_right_logical(offs, 6), lax.bitwise_and(offs, 63)
    parts = jnp.where(row == 0, hi, jnp.where(row == 1, lo, 0)).astype(F32).astype(BF16)
    got = dot(parts, pick, 1, 1).astype(I32)
    return got[0:1] * 64 + got[1:2]


def step_kernel(group, scale, fid_hbm, x_hbm, n1_hbm, n2_hbm, lab_hbm, ws1_hbm, wn1_hbm, ws2_hbm, wn2_hbm, r_ref,
                fid_ref, x_ref, n1_ref, n2_ref, lab_ref, ws1_ref, wn1_ref, ws2_ref, wn2_ref, in_sem,
                ws1_t, wn1_t, ws2_t, wn2_t, ask, ask_in, rep, rep_in, hsend, hrecv, up,
                small, idx, acc, nf, both, z_ref, gpad, g,
                rc, part, l1a, l1b, w2a, w2b, l2a, l2b, zc, lz, zg, send, recv):
    nx, ny, nz = dims_of(group)
    ca, cb = chunks_of(group)
    cx, cy, zn = ny * ca, nx * cb, ca + cb
    nq = max(1, nz // 2)
    zsize = -(-zn // nq)
    off_b = nx * cx
    half = off_b + ny * cy
    me = lax.axis_index('g')
    core = lax.rem(me, 2)
    mx = lax.rem(me // 2, nx)
    my = lax.rem(me // (2 * nx), ny)
    mz = me // (2 * nx * ny)

    def dev(z, y, x, c):
        return ((z * ny + y) * nx + x) * 2 + c

    mate = dev(mz, my, mx, 1 - core)
    xs = [lax.rem(mx + d, nx) for d in range(nx)]
    ys = [lax.rem(my + d, ny) for d in range(ny)]
    zs = [lax.rem(mz + d, nz) for d in range(nz)]
    xdev = [dev(mz, my, x, core) for x in xs]
    ydev = [dev(mz, y, mx, core) for y in ys]
    zdev = [dev(z, my, mx, core) for z in zs]
    left, right = lax.rem(me + group - 1, group), lax.rem(me + 1, group)

    barrier = pltpu.get_barrier_semaphore()
    peers = [left, right, mate] + xdev[1:] + ydev[1:]

    def signal(sem, to):
        pl.semaphore_signal(sem, inc=1, device_id=(to,), device_id_type=MESH)

    for nb in peers:
        pl.semaphore_signal(barrier, inc=1, device_id=(nb,), device_id_type=MESH)
    for d in range(1, nz):
        pl.when(mz + d < nz)(functools.partial(signal, barrier, zdev[d]))
    loads = [pltpu.make_async_copy(src, dst, in_sem.at[i]) for i, (src, dst) in
             enumerate(((fid_hbm, fid_ref), (n1_hbm, n1_ref), (x_hbm, x_ref), (n2_hbm, n2_ref), (lab_hbm, lab_ref),
                        (ws1_hbm, ws1_ref), (wn1_hbm, wn1_ref), (ws2_hbm, ws2_ref), (wn2_hbm, wn2_ref)))]
    for cp in loads:
        cp.start()

    feat, store = x_ref.shape
    targets = n1_ref.shape[1]
    fan_one = n1_ref.shape[0]
    fan_two, seeds = n2_ref.shape
    classes = ws2_ref.shape[0]
    width = acc.shape[0]
    hrows = rep.shape[1]
    loads[0].wait()
    ext, off = frontier_ext(fid_ref[...], me, group, store.bit_length() - 1)
    ask[...] = jnp.broadcast_to(ask_rows(ext, off, store), ask.shape)
    asks = []
    for i, nb in enumerate((left, right)):
        asks.append(pltpu.make_async_remote_copy(ask, ask_in.at[i], hsend.at[i], hrecv.at[i], device_id=(nb,), device_id_type=MESH))

    def ask_neighbours():
        pl.semaphore_wait(barrier, len(peers) + mz)
        for cp in asks:
            cp.start()
        for d in range(1, nz):
            pl.when(mz + d >= nz)(functools.partial(signal, up.at[nz - d], zdev[d]))

    first_of_plane = lax.rem(me, 2 * nx * ny) == 0
    pl.when(jnp.logical_not(first_of_plane))(ask_neighbours)

    loads[1].wait()
    for r0 in range(0, fan_one, 8):
        nr = min(8, fan_one - r0)
        for c0 in range(0, targets, 128):
            pos = n1_ref[r0:r0 + nr, c0:c0 + 128]
            if nr < 8:
                pos = jnp.broadcast_to(pos[0:1], (8, 128)) if nr == 1 else jnp.concatenate([pos, pos[0:8 - nr]], axis=0)
            hi = lax.shift_right_logical(pos, 7)
            lo = lax.bitwise_and(pos, 127)
            val = jnp.zeros((8, 128), I32)
            for h in range(ext.shape[0]):
                row = jnp.broadcast_to(ext[h:h + 1, :], (8, 128))
                val = jnp.where(hi == h, jnp.take_along_axis(row, lo, axis=1, mode='promise_in_bounds'), val)
            fld = jnp.zeros((8, 128), I32)
            for f in range(1, FIELDS):
                fld = fld + jnp.where(val >= f * width, 1, 0)
            idx[0, r0:r0 + 8, c0:c0 + 128] = val - fld * width
            idx[1, r0:r0 + 8, c0:c0 + 128] = lax.shift_left(jnp.ones((8, 128), I32), fld * FIELD_BITS)
    first = lanes_of(ext[0:targets // 128, :])
    nf[:, 0:targets] = jnp.where(iota((nf.shape[0], targets), 0) == first, 1.0, 0.0).astype(BF16)

    block = 16

    def count_block(b, carry):
        base = pl.multiple_of(b * block, block)
        for c0 in range(0, targets, 256):
            row = iota((block, 256), 0) + base
            tot = jnp.zeros((block, 256), I32)
            for k in range(fan_one):
                tot = tot + jnp.where(row == idx[0, k:k + 1, c0:c0 + 256], idx[1, k:k + 1, c0:c0 + 256], 0)
            acc[pl.ds(base, block), c0:c0 + 256] = tot
        return carry

    lax.fori_loop(0, width // block, count_block, 0)
    for f in range(FIELDS):
        cnt = lax.bitwise_and(lax.shift_right_logical(acc[...], f * FIELD_BITS), (1 << FIELD_BITS) - 1)
        nf[f * width:(f + 1) * width, targets:2 * targets] = cnt.astype(F32).astype(BF16)

    for cp in loads[3:]:
        cp.wait()
    small[...] = jnp.full(small.shape, -1, I32)
    small[0:fan_two, 0:seeds] = n2_ref[...]
    small[12:13, 0:seeds] = lab_ref[...]
    m2 = jnp.zeros((targets, 128), F32)
    for k in range(fan_two):
        m2 = m2 + jnp.where(iota((targets, 128), 0) == small[k:k + 1, :], 1.0, 0.0)
    m2 = m2.astype(BF16)
    for src, dst in ((ws1_ref, ws1_t), (wn1_ref, wn1_t), (ws2_ref, ws2_t), (wn2_ref, wn2_t)):
        dst[...] = src[...].T

    pl.when(first_of_plane)(ask_neighbours)

    for cp in asks:
        cp.wait_recv()
    lane = iota((1, 128), 1)
    want = jnp.where(lane < HALO, ask_in[0, 0:1, :], ask_in[1, 0:1, :])
    pick = jnp.where(iota((store, 128), 0) == want, 1.0, 0.0).astype(BF16)
    loads[2].wait()
    reps = []
    cut = 16 * (hrows // 32 + 1)
    for i, (lo, n) in enumerate(((0, cut), (cut, hrows - cut))):
        out = dot(x_ref[2 * lo:min(2 * lo + 2 * n, feat), :], pick)
        if out.shape[0] < 2 * n:
            out = jnp.concatenate([out, jnp.zeros((2 * n - out.shape[0], 128), F32)], axis=0)
        top, bot = out[0:n], out[n:2 * n]
        low = iota((n, 128), 1) < HALO
        rep[0, lo:lo + n] = jnp.where(low, top, pltpu.roll(bot, HALO, 1)).astype(BF16)
        rep[1, lo:lo + n] = jnp.where(low, pltpu.roll(top, HALO, 1), bot).astype(BF16)
        for k, nb in enumerate((right, left)):
            reps.append(pltpu.make_async_remote_copy(rep.at[k, lo:lo + n], rep_in.at[k, lo:lo + n], hsend.at[2 + 2 * i + k],
                                                     hrecv.at[2 + 2 * i + k], device_id=(nb,), device_id_type=MESH))
            reps[-1].start()

    both[...] = dot(x_ref[...], nf[0:store, :])

    for cp in reps:
        cp.wait_recv()
    halves = []
    for lo, n in ((0, cut), (cut, hrows - cut)):
        low = iota((n, 128), 1) < HALO
        from_l, from_r = rep_in[0, lo:lo + n].astype(F32), rep_in[1, lo:lo + n].astype(F32)
        halves += [jnp.where(low, from_l, pltpu.roll(from_r, HALO, 1)).astype(BF16),
                   jnp.where(low, pltpu.roll(from_l, HALO, 1), from_r).astype(BF16)]
    halo = jnp.concatenate(halves, axis=0)
    rows = both[...] + dot(halo[0:feat], nf[store:store + 2 * HALO, :])
    x_t = rows[:, 0:targets].astype(BF16)
    a_t = (rows[:, targets:] * (1.0 / fan_one)).astype(BF16)
    z = dot(ws1_t[...], x_t) + dot(wn1_t[...], a_t)
    z_ref[...] = z
    h = jnp.maximum(z, 0.0).astype(BF16)
    a2 = (dot(h, m2) * (1.0 / fan_two)).astype(BF16)
    hs = h[:, 0:128]
    ws2, wn2 = ws2_ref[...], wn2_ref[...]
    logits = dot(ws2, hs) + dot(wn2, a2)
    shifted = logits - jnp.max(logits, axis=0, keepdims=True)
    log_prob = shifted - jnp.log(jnp.sum(jnp.exp(shifted), axis=0, keepdims=True))
    hit = iota(logits.shape, 0) == small[12:13, :]
    loss = -jnp.sum(jnp.where(hit, log_prob, 0.0))
    gl = (jnp.exp(log_prob) - jnp.where(hit, 1.0, 0.0)) * scale
    gpad[...] = jnp.zeros(gpad.shape, F32)
    gpad[0:classes, :] = jnp.where(lane < seeds, gl, 0.0)
    gb = gpad[...].astype(BF16)
    d_s2 = dot(gb, hs, 1, 1)
    d_n2 = dot(gb, a2, 1, 1)
    d_s2 = jnp.where(iota(d_s2.shape, 0) == classes, loss, d_s2)
    gc = gb[0:classes]
    g_seed = dot(ws2_t[...], gc)
    g_agg = dot(wn2_t[...], gc) * (1.0 / fan_two)
    p0 = g_agg.astype(BF16)
    r1 = g_agg - p0.astype(F32)
    p1 = r1.astype(BF16)
    p2 = (r1 - p1.astype(F32)).astype(BF16)
    d_h = dot(p0, m2, 1, 1) + (dot(p1, m2, 1, 1) + dot(p2, m2, 1, 1))
    d_h = d_h + jnp.concatenate([g_seed, jnp.zeros((g_seed.shape[0], targets - 128), F32)], axis=1)
    d_z = jnp.where(z_ref[...] > 0, d_h, 0.0).astype(BF16)
    tail = jnp.zeros((2 * hrows - feat, d_z.shape[0]), F32)
    at = 0
    for mat in (jnp.concatenate([dot(x_t, d_z, 1, 1), tail], axis=0),
                jnp.concatenate([dot(a_t, d_z, 1, 1), tail], axis=0), d_s2, d_n2):
        n = mat.shape[0] // 8
        for c0 in range(0, mat.shape[1], 128):
            g[at:at + n] = mat[:, c0:c0 + 128].reshape(n, 8, 128)
            at += n
    if at < g.shape[0]:
        g[at:] = jnp.zeros((g.shape[0] - at, 8, 128), F32)

    copies = []

    def put(src, dst, to):
        k = len(copies)
        cp = pltpu.make_async_remote_copy(src, dst, send.at[k], recv.at[k], device_id=(to,), device_id_type=MESH)
        cp.start()
        copies.append(cp)
        return cp

    other, mine = (1 - core) * half, core * half
    part_a = (nx, xs, xdev, cx, 0, ny, ys, ydev, ca, l1a, w2a, l2a)
    part_b = (ny, ys, ydev, cy, off_b, nx, xs, xdev, cb, l1b, w2b, l2b)
    parts = (part_a, part_b)
    pieces = []
    for i in range(max(nx, ny)):
        for w, p in enumerate(parts):
            if i < p[0]:
                d = far_first(p[0])[i]
                pieces.append((w, d, p[4] + p[1][d] * p[3]))
    arrive = [put(g.at[pl.ds(other + o, parts[w][3])], rc.at[pl.ds(o, parts[w][3])], mate) for w, d, o in pieces]
    first_in = [{}, {}]
    for (w, d, o), cp in zip(pieces, arrive):
        _, _, to, n, _, n2, sub, _, c, land, _, _ = parts[w]
        cp.wait_recv()
        part[pl.ds(o, n)] = g[pl.ds(mine + o, n)] + rc[pl.ds(o, n)]
        if d:
            for i in range(n2):
                e = far_first(n2)[i]
                first_in[w][d, e] = put(part.at[pl.ds(o + sub[e] * c, c)], land.at[d - 1, e], to[d])
    second_in, sums = [[], []], [None, None]
    for i in range(max(nx, ny)):
        for w, (n1, own, _, n, off, n2, sub, to, c, land, w2, l2) in enumerate(parts):
            if i < n2:
                e = far_first(n2)[i]
                tot = part[pl.ds(off + own[0] * n + sub[e] * c, c)]
                for d in range(1, n1):
                    first_in[w][d, e].wait_recv()
                    tot = tot + land[d - 1, e]
                if e:
                    w2[e - 1] = tot
                    second_in[w].append((e, put(w2.at[e - 1], l2.at[e - 1], to[e])))
                else:
                    sums[w] = tot
    for w, at, n in ((0, 0, ca), (1, ca, cb)):
        tot = sums[w]
        for e, cp in second_in[w]:
            cp.wait_recv()
            tot = tot + parts[w][11][e - 1]
        zc[at:at + n] = tot
    for d in range(1, nz):
        pl.when(mz + d < nz)(functools.partial(pl.semaphore_wait, up.at[d], 1))
    quarter = lax.rem(mz, nq)
    in_z = [put(zc.at[pl.ds((zn * lax.rem(zs[d], nq)) // nq, zsize)], lz.at[mz], zdev[d]) for d in far_first(nz)[:-1]]
    lz[mz] = zc[pl.ds((zn * quarter) // nq, zsize)]
    for cp in in_z:
        cp.wait_recv()
    tot = lz[0]
    for z in range(1, nz):
        tot = tot + lz[z]
    zg[quarter] = tot
    done = 0
    if nq == 4:
        far = lax.rem(mz + 2 + 4 * lax.rem(mz, 2), nz)
        targets_z = (dev(far, my, mx, core), zdev[1], zdev[nz - 1])
        done = list(copies) + asks + reps
        in_z = [put(zg.at[quarter], zg.at[quarter], to) for to in targets_z]
        for cp in done:
            cp.wait_send()
        done = len(copies) - 3
        for cp in in_z:
            cp.wait_recv()
    base = [mine + p[4] + p[1][0] * p[3] for p in parts]
    spots = [base[w] + p[6][0] * p[8] for w, p in enumerate(parts)]
    for q in range(nq):
        lo = (zn * q) // nq
        end = (zn * (q + 1)) // nq
        for t in range(lo, end):
            at = spots[0] + t if t < ca else spots[1] + (t - ca)
            r_ref[pl.ds(at, 1)] = zg[q, t - lo:t - lo + 1]
    back = []

    def spread(w, at):
        n1, _, to, _, _, _, _, _, c, _, _, _ = parts[w]
        got = {d: put(r_ref.at[pl.ds(at, c)], r_ref.at[pl.ds(at, c)], to[d]) for d in far_first(n1)[:-1]}
        back.append(put(r_ref.at[pl.ds(at, c)], r_ref.at[pl.ds(at, c)], mate))
        return got

    second_in = [{}, {}]
    for w, p in enumerate(parts):
        for e in far_first(p[5])[:-1]:
            second_in[w][e] = (put(r_ref.at[pl.ds(spots[w], p[8])], r_ref.at[pl.ds(spots[w], p[8])], p[7][e]))
    first_in = [[spread(w, spots[w])] for w in range(2)]
    for i in range(max(nx, ny)):
        for w, (n1, own, _, n, off, n2, sub, _, c, _, _, _) in enumerate(parts):
            if i < n2 - 1:
                e = far_first(n2)[n2 - 2 - i]
                second_in[w][e].wait_recv()
                first_in[w].append(spread(w, base[w] + sub[n2 - e] * c))
    for cp in copies[done:] + ([] if done else asks + reps):
        cp.wait_send()
    sent = len(copies)
    for i in range(max(nx, ny)):
        for w, (n1, own, _, n, off, n2, sub, _, c, _, _, _) in enumerate(parts):
            if i < n2:
                e = far_first(n2)[n2 - 1 - i]
                for d in reversed(far_first(n1)[:-1]):
                    first_in[w][i][d].wait_recv()
                    at = mine + off + own[n1 - d] * n + sub[(n2 - e) % n2] * c
                    back.append(put(r_ref.at[pl.ds(at, c)], r_ref.at[pl.ds(at, c)], mate))
    for cp in back:
        cp.wait_recv()
    for cp in copies[sent:]:
        cp.wait_send()


def copy_count(group):
    nx, ny, nz = dims_of(group)
    return nx + ny + 2 * ((nx - 1) * ny + (ny - 1) * nx + nx - 1 + ny - 1) + nz - 1 + (3 if nz == 8 else 0) + 2 * nx * ny


def output_kernel(scale, r_ref, loss_ref, s1_hbm, n1_hbm, s2_hbm, n2_hbm, s1, n1, s2, n2, sem):
    at, k = 0, 0
    classes = s2.shape[0]
    copies = []
    for ref, hbm in ((s1, s1_hbm), (n1, n1_hbm), (s2, s2_hbm), (n2, n2_hbm)):
        rows, cols = ref.shape
        n = -(-rows // 8)
        step = n if n < 16 else 19
        for r0 in range(0, n, step):
            lo, hi = r0 * 8, min(rows, (r0 + step) * 8)
            for c in range(cols // 128):
                val = r_ref[at + c * n + r0:at + c * n + r0 + step].reshape(step * 8, 128)
                ref[lo:hi, c * 128:(c + 1) * 128] = val[0:hi - lo]
                if ref is s2 and c == 0:
                    loss_ref[...] = val[classes:classes + 1, 0:1] * scale
            cp = pltpu.make_async_copy(ref.at[lo:hi], hbm.at[lo:hi], sem.at[k])
            cp.start()
            copies.append(cp)
            k += 1
        at += n * (cols // 128)
    for cp in copies:
        cp.wait()


def solution(mesh):
    group = mesh.shape['g']

    def device_step(x_local, front_ids, nbr_one, nbr_two, labels, w_self1, w_nbr1, w_self2, w_nbr2):
        store, feat = x_local.shape
        targets, fan_one = nbr_one.shape
        seeds, fan_two = nbr_two.shape
        hidden, classes = w_self2.shape
        frows = -(-feat // 32) * 32
        scale = 1.0 / (group * seeds)
        fid = front_ids.reshape(-1, 128)
        width = -(-(store + 2 * HALO) // (FIELDS * 16)) * 16
        nx, ny, nz = dims_of(group)
        ca, cb = chunks_of(group)
        cx, cy, zn = ny * ca, nx * cb, ca + cb
        nq = max(1, nz // 2)
        zsize = -(-zn // nq)
        half = nx * cx + ny * cy
        total = 2 * half
        n = copy_count(group)
        dma = pltpu.SemaphoreType.DMA

        def buf(*lead):
            return VMEM((*lead, 8, 128), F32)

        vm, hbm = pl.BlockSpec(memory_space=VMEM), pl.BlockSpec(memory_space=pl.ANY)
        sums = pl.pallas_call(
            functools.partial(step_kernel, group, scale),
            name='train_step',
            out_shape=VMEM((total, 8, 128), F32),
            in_specs=[hbm] * 9,
            out_specs=vm,
            scratch_shapes=[
                VMEM(fid.shape, I32), VMEM((feat, store), BF16), VMEM((fan_one, targets), I32), VMEM((fan_two, seeds), I32),
                VMEM((1, seeds), I32), VMEM((feat, hidden), BF16), VMEM((feat, hidden), BF16), VMEM((classes, hidden), BF16),
                VMEM((classes, hidden), BF16), dma((9,)),
                VMEM((hidden, feat), BF16), VMEM((hidden, feat), BF16), VMEM((hidden, classes), BF16), VMEM((hidden, classes), BF16),
                VMEM((8, 128), I32), VMEM((2, 8, 128), I32), VMEM((2, frows // 2, 128), BF16),
                VMEM((2, frows // 2, 128), BF16), dma((6,)), dma((6,)),
                pltpu.SemaphoreType.REGULAR((nz,)),
                VMEM((16, 128), I32), VMEM((2, -(-fan_one // 8) * 8, targets), I32), VMEM((width, targets), I32),
                VMEM((FIELDS * width, 2 * targets), BF16), VMEM((feat, 2 * targets), F32), VMEM((hidden, targets), F32),
                VMEM((-(-classes // 16) * 16, 128), F32), buf(total),
                buf(half), buf(half), buf(nx - 1, ny, ca), buf(ny - 1, nx, cb), buf(ny - 1, ca), buf(nx - 1, cb),
                buf(ny - 1, ca), buf(nx - 1, cb), buf(zn), buf(nz, zsize), buf(nq, zsize),
                dma((n,)), dma((n,))],
            compiler_params=pltpu.CompilerParams(collective_id=0, has_side_effects=True,
                                                 vmem_limit_bytes=60 * 1024 * 1024),
        )(fid, x_local.T, nbr_one.T, nbr_two.T, labels.reshape(1, -1), w_self1, w_nbr1, w_self2.T, w_nbr2.T)
        loss, d_s1, d_n1, d_s2, d_n2 = pl.pallas_call(
            functools.partial(output_kernel, scale),
            name='split_outputs',
            out_shape=[jax.ShapeDtypeStruct((1, 1), F32), jax.ShapeDtypeStruct((feat, hidden), F32),
                       jax.ShapeDtypeStruct((feat, hidden), F32), jax.ShapeDtypeStruct((classes, hidden), F32),
                       jax.ShapeDtypeStruct((classes, hidden), F32)],
            in_specs=[vm], out_specs=[vm] + [hbm] * 4,
            scratch_shapes=[VMEM((feat, hidden), F32), VMEM((feat, hidden), F32), VMEM((classes, hidden), F32),
                            VMEM((classes, hidden), F32), dma((10,))],
        )(pltpu.with_memory_space_constraint(sums, VMEM))
        return loss[0, 0], d_s1, d_n1, d_s2.T, d_n2.T

    return jax.shard_map(device_step, mesh=mesh,
                         in_specs=(P('g', None), P('g'), P('g', None), P('g', None), P('g'), P(), P(), P(), P()),
                         out_specs=(P(), P(), P(), P(), P()), check_vma=False)
```

```python
import functools

import jax
import jax.numpy as jnp
from jax import lax
from jax.experimental import pallas as pl
from jax.experimental.pallas import tpu as pltpu
from jax.sharding import PartitionSpec as P

MESH = pl.DeviceIdType.MESH
F32, BF16, I32 = jnp.float32, jnp.bfloat16, jnp.int32
VMEM = pltpu.VMEM

HALO = 64
FIELDS, FIELD_BITS = 6, 5


def dims_of(group):
    return {256: (4, 4, 8), 16: (2, 2, 2)}[group]


def chunks_of(group):
    return {256: (6, 5), 16: (21, 20)}[group]


def dot(a, b, ca=1, cb=0):
    return lax.dot_general(a, b, (((ca,), (cb,)), ((), ())), preferred_element_type=F32)


def iota(shape, dim):
    return lax.broadcasted_iota(I32, shape, dim)


def far_first(n):
    return sorted(range(1, n), key=lambda d: -min(d, n - d)) + [0]


def frontier_ext(fid, me, group, rows_log2):
    store = 1 << rows_log2
    owner = lax.shift_right_logical(fid, rows_log2)
    off = lax.bitwise_and(fid, store - 1)
    left, right = lax.rem(me + group - 1, group), lax.rem(me + 1, group)
    is_l, is_r = owner == left, owner == right
    mask = jnp.concatenate([jnp.where(is_l, 1.0, 0.0), jnp.where(is_r, 1.0, 0.0)], axis=0).astype(BF16)
    n = fid.shape[0]
    upper = jnp.where(iota((128, 128), 0) < iota((128, 128), 1), 1.0, 0.0).astype(BF16)
    ri, ci = iota((2 * n, 2 * n), 0), iota((2 * n, 2 * n), 1)
    before = jnp.where((ci < ri) & ((ci < n) == (ri < n)), 1.0, 0.0).astype(BF16)
    ones = jnp.ones((128, 128), BF16)
    rank = dot(mask, upper) + dot(dot(before, mask).astype(BF16), ones)
    rank = rank.astype(I32)
    rank_l, rank_r = rank[:n], rank[n:]
    ext = jnp.where(is_l, store + rank_l, jnp.where(is_r, store + HALO + rank_r, off))
    return ext, off


def lanes_of(a):
    return jnp.concatenate([a[i:i + 1, :] for i in range(a.shape[0])], axis=1)


def ask_rows(ext, off, store):
    key = lanes_of(ext) - store
    offs = lanes_of(off)
    pick = jnp.where(iota((2 * HALO, key.shape[1]), 0) == key, 1.0, 0.0).astype(BF16)
    row = iota((16, key.shape[1]), 0)
    hi, lo = lax.shift_right_logical(offs, 6), lax.bitwise_and(offs, 63)
    parts = jnp.where(row == 0, hi, jnp.where(row == 1, lo, 0)).astype(F32).astype(BF16)
    got = dot(parts, pick, 1, 1).astype(I32)
    return got[0:1] * 64 + got[1:2]


def step_kernel(group, scale, fid_hbm, x_hbm, n1_hbm, n2_hbm, lab_hbm, ws1_hbm, wn1_hbm, ws2_hbm, wn2_hbm, r_ref,
                fid_ref, x_ref, n1_ref, n2_ref, lab_ref, ws1_ref, wn1_ref, ws2_ref, wn2_ref, in_sem,
                ws1_t, wn1_t, ws2_t, wn2_t, ask, ask_in, rep, rep_in, hsend, hrecv, up,
                small, idx, acc, nf, both, z_ref, gpad, g,
                rc, part, l1a, l1b, w2a, w2b, l2a, l2b, zc, lz, zg, send, recv):
    nx, ny, nz = dims_of(group)
    ca, cb = chunks_of(group)
    cx, cy, zn = ny * ca, nx * cb, ca + cb
    nq = max(1, nz // 2)
    zsize = -(-zn // nq)
    off_b = nx * cx
    half = off_b + ny * cy
    me = lax.axis_index('g')
    core = lax.rem(me, 2)
    mx = lax.rem(me // 2, nx)
    my = lax.rem(me // (2 * nx), ny)
    mz = me // (2 * nx * ny)

    def dev(z, y, x, c):
        return ((z * ny + y) * nx + x) * 2 + c

    mate = dev(mz, my, mx, 1 - core)
    xs = [lax.rem(mx + d, nx) for d in range(nx)]
    ys = [lax.rem(my + d, ny) for d in range(ny)]
    zs = [lax.rem(mz + d, nz) for d in range(nz)]
    xdev = [dev(mz, my, x, core) for x in xs]
    ydev = [dev(mz, y, mx, core) for y in ys]
    zdev = [dev(z, my, mx, core) for z in zs]
    left, right = lax.rem(me + group - 1, group), lax.rem(me + 1, group)

    barrier = pltpu.get_barrier_semaphore()
    peers = [left, right, mate] + xdev[1:] + ydev[1:]

    def signal(sem, to):
        pl.semaphore_signal(sem, inc=1, device_id=(to,), device_id_type=MESH)

    for nb in peers:
        pl.semaphore_signal(barrier, inc=1, device_id=(nb,), device_id_type=MESH)
    for d in range(1, nz):
        pl.when(mz + d < nz)(functools.partial(signal, barrier, zdev[d]))
    loads = [pltpu.make_async_copy(src, dst, in_sem.at[i]) for i, (src, dst) in
             enumerate(((fid_hbm, fid_ref), (n1_hbm, n1_ref), (x_hbm, x_ref), (n2_hbm, n2_ref), (lab_hbm, lab_ref),
                        (ws1_hbm, ws1_ref), (wn1_hbm, wn1_ref), (ws2_hbm, ws2_ref), (wn2_hbm, wn2_ref)))]
    for cp in loads:
        cp.start()

    feat, store = x_ref.shape
    targets = n1_ref.shape[1]
    fan_one = n1_ref.shape[0]
    fan_two, seeds = n2_ref.shape
    classes = ws2_ref.shape[0]
    width = acc.shape[0]
    hrows = rep.shape[1]
    loads[0].wait()
    ext, off = frontier_ext(fid_ref[...], me, group, store.bit_length() - 1)
    ask[...] = jnp.broadcast_to(ask_rows(ext, off, store), ask.shape)
    asks = []
    for i, nb in enumerate((left, right)):
        asks.append(pltpu.make_async_remote_copy(ask, ask_in.at[i], hsend.at[i], hrecv.at[i], device_id=(nb,), device_id_type=MESH))

    def ask_neighbours():
        pl.semaphore_wait(barrier, len(peers) + mz)
        for cp in asks:
            cp.start()
        for d in range(1, nz):
            pl.when(mz + d >= nz)(functools.partial(signal, up.at[nz - d], zdev[d]))

    first_of_plane = lax.rem(me, 2 * nx * ny) == 0
    pl.when(jnp.logical_not(first_of_plane))(ask_neighbours)

    loads[1].wait()
    for r0 in range(0, fan_one, 8):
        nr = min(8, fan_one - r0)
        for c0 in range(0, targets, 128):
            pos = n1_ref[r0:r0 + nr, c0:c0 + 128]
            if nr < 8:
                pos = jnp.broadcast_to(pos[0:1], (8, 128)) if nr == 1 else jnp.concatenate([pos, pos[0:8 - nr]], axis=0)
            hi = lax.shift_right_logical(pos, 7)
            lo = lax.bitwise_and(pos, 127)
            val = jnp.zeros((8, 128), I32)
            for h in range(ext.shape[0]):
                row = jnp.broadcast_to(ext[h:h + 1, :], (8, 128))
                val = jnp.where(hi == h, jnp.take_along_axis(row, lo, axis=1, mode='promise_in_bounds'), val)
            fld = jnp.zeros((8, 128), I32)
            for f in range(1, FIELDS):
                fld = fld + jnp.where(val >= f * width, 1, 0)
            idx[0, r0:r0 + 8, c0:c0 + 128] = val - fld * width
            idx[1, r0:r0 + 8, c0:c0 + 128] = lax.shift_left(jnp.ones((8, 128), I32), fld * FIELD_BITS)
    first = lanes_of(ext[0:targets // 128, :])
    nf[:, 0:targets] = jnp.where(iota((nf.shape[0], targets), 0) == first, 1.0, 0.0).astype(BF16)

    block = 16

    def count_block(b, carry):
        base = pl.multiple_of(b * block, block)
        for c0 in range(0, targets, 256):
            row = iota((block, 256), 0) + base
            tot = jnp.zeros((block, 256), I32)
            for k in range(fan_one):
                tot = tot + jnp.where(row == idx[0, k:k + 1, c0:c0 + 256], idx[1, k:k + 1, c0:c0 + 256], 0)
            acc[pl.ds(base, block), c0:c0 + 256] = tot
        return carry

    lax.fori_loop(0, width // block, count_block, 0)
    for f in range(FIELDS):
        cnt = lax.bitwise_and(lax.shift_right_logical(acc[...], f * FIELD_BITS), (1 << FIELD_BITS) - 1)
        nf[f * width:(f + 1) * width, targets:2 * targets] = cnt.astype(F32).astype(BF16)

    for cp in loads[3:]:
        cp.wait()
    small[...] = jnp.full(small.shape, -1, I32)
    small[0:fan_two, 0:seeds] = n2_ref[...]
    small[12:13, 0:seeds] = lab_ref[...]
    m2 = jnp.zeros((targets, 128), F32)
    for k in range(fan_two):
        m2 = m2 + jnp.where(iota((targets, 128), 0) == small[k:k + 1, :], 1.0, 0.0)
    m2 = m2.astype(BF16)
    for src, dst in ((ws1_ref, ws1_t), (wn1_ref, wn1_t), (ws2_ref, ws2_t), (wn2_ref, wn2_t)):
        dst[...] = src[...].T

    pl.when(first_of_plane)(ask_neighbours)

    for cp in asks:
        cp.wait_recv()
    lane = iota((1, 128), 1)
    want = jnp.where(lane < HALO, ask_in[0, 0:1, :], ask_in[1, 0:1, :])
    pick = jnp.where(iota((store, 128), 0) == want, 1.0, 0.0).astype(BF16)
    loads[2].wait()
    reps = []
    cuts = [(0, 112), (112, 96), (208, hrows - 208)]
    for i, (lo, n) in enumerate(cuts):
        out = dot(x_ref[2 * lo:min(2 * lo + 2 * n, feat), :], pick)
        if out.shape[0] < 2 * n:
            out = jnp.concatenate([out, jnp.zeros((2 * n - out.shape[0], 128), F32)], axis=0)
        top, bot = out[0:n], out[n:2 * n]
        low = iota((n, 128), 1) < HALO
        rep[0, lo:lo + n] = jnp.where(low, top, pltpu.roll(bot, HALO, 1)).astype(BF16)
        rep[1, lo:lo + n] = jnp.where(low, pltpu.roll(top, HALO, 1), bot).astype(BF16)
        for k, nb in enumerate((right, left)):
            reps.append(pltpu.make_async_remote_copy(rep.at[k, lo:lo + n], rep_in.at[k, lo:lo + n], hsend.at[2 + 2 * i + k],
                                                     hrecv.at[2 + 2 * i + k], device_id=(nb,), device_id_type=MESH))
            reps[-1].start()

    both[...] = dot(x_ref[...], nf[0:store, :])

    for cp in reps:
        cp.wait_recv()
    halves = []
    for lo, n in cuts:
        low = iota((n, 128), 1) < HALO
        from_l, from_r = rep_in[0, lo:lo + n].astype(F32), rep_in[1, lo:lo + n].astype(F32)
        halves += [jnp.where(low, from_l, pltpu.roll(from_r, HALO, 1)).astype(BF16),
                   jnp.where(low, pltpu.roll(from_l, HALO, 1), from_r).astype(BF16)]
    halo = jnp.concatenate(halves, axis=0)
    rows = both[...] + dot(halo[0:feat], nf[store:store + 2 * HALO, :])
    x_t = rows[:, 0:targets].astype(BF16)
    a_t = (rows[:, targets:] * (1.0 / fan_one)).astype(BF16)
    z = dot(ws1_t[...], x_t) + dot(wn1_t[...], a_t)
    z_ref[...] = z
    h = jnp.maximum(z, 0.0).astype(BF16)
    a2 = (dot(h, m2) * (1.0 / fan_two)).astype(BF16)
    hs = h[:, 0:128]
    ws2, wn2 = ws2_ref[...], wn2_ref[...]
    logits = dot(ws2, hs) + dot(wn2, a2)
    shifted = logits - jnp.max(logits, axis=0, keepdims=True)
    log_prob = shifted - jnp.log(jnp.sum(jnp.exp(shifted), axis=0, keepdims=True))
    hit = iota(logits.shape, 0) == small[12:13, :]
    loss = -jnp.sum(jnp.where(hit, log_prob, 0.0))
    gl = (jnp.exp(log_prob) - jnp.where(hit, 1.0, 0.0)) * scale
    gpad[...] = jnp.zeros(gpad.shape, F32)
    gpad[0:classes, :] = jnp.where(lane < seeds, gl, 0.0)
    gb = gpad[...].astype(BF16)
    d_s2 = dot(gb, hs, 1, 1)
    d_n2 = dot(gb, a2, 1, 1)
    d_s2 = jnp.where(iota(d_s2.shape, 0) == classes, loss, d_s2)
    gc = gb[0:classes]
    g_seed = dot(ws2_t[...], gc)
    g_agg = dot(wn2_t[...], gc) * (1.0 / fan_two)
    p0 = g_agg.astype(BF16)
    r1 = g_agg - p0.astype(F32)
    p1 = r1.astype(BF16)
    p2 = (r1 - p1.astype(F32)).astype(BF16)
    d_h = dot(p0, m2, 1, 1) + (dot(p1, m2, 1, 1) + dot(p2, m2, 1, 1))
    d_h = d_h + jnp.concatenate([g_seed, jnp.zeros((g_seed.shape[0], targets - 128), F32)], axis=1)
    d_z = jnp.where(z_ref[...] > 0, d_h, 0.0).astype(BF16)
    tail = jnp.zeros((2 * hrows - feat, d_z.shape[0]), F32)
    at = 0
    for mat in (jnp.concatenate([dot(x_t, d_z, 1, 1), tail], axis=0),
                jnp.concatenate([dot(a_t, d_z, 1, 1), tail], axis=0), d_s2, d_n2):
        n = mat.shape[0] // 8
        for c0 in range(0, mat.shape[1], 128):
            g[at:at + n] = mat[:, c0:c0 + 128].reshape(n, 8, 128)
            at += n
    if at < g.shape[0]:
        g[at:] = jnp.zeros((g.shape[0] - at, 8, 128), F32)

    copies = []

    def put(src, dst, to):
        k = len(copies)
        cp = pltpu.make_async_remote_copy(src, dst, send.at[k], recv.at[k], device_id=(to,), device_id_type=MESH)
        cp.start()
        copies.append(cp)
        return cp

    other, mine = (1 - core) * half, core * half
    part_a = (nx, xs, xdev, cx, 0, ny, ys, ydev, ca, l1a, w2a, l2a)
    part_b = (ny, ys, ydev, cy, off_b, nx, xs, xdev, cb, l1b, w2b, l2b)
    parts = (part_a, part_b)
    pieces = []
    for i in range(max(nx, ny)):
        for w, p in enumerate(parts):
            if i < p[0]:
                d = far_first(p[0])[i]
                pieces.append((w, d, p[4] + p[1][d] * p[3]))
    arrive = [put(g.at[pl.ds(other + o, parts[w][3])], rc.at[pl.ds(o, parts[w][3])], mate) for w, d, o in pieces]
    first_in = [{}, {}]
    for (w, d, o), cp in zip(pieces, arrive):
        _, _, to, n, _, n2, sub, _, c, land, _, _ = parts[w]
        cp.wait_recv()
        part[pl.ds(o, n)] = g[pl.ds(mine + o, n)] + rc[pl.ds(o, n)]
        if d:
            for i in range(n2):
                e = far_first(n2)[i]
                first_in[w][d, e] = put(part.at[pl.ds(o + sub[e] * c, c)], land.at[d - 1, e], to[d])
    second_in, sums = [[], []], [None, None]
    for i in range(max(nx, ny)):
        for w, (n1, own, _, n, off, n2, sub, to, c, land, w2, l2) in enumerate(parts):
            if i < n2:
                e = far_first(n2)[i]
                tot = part[pl.ds(off + own[0] * n + sub[e] * c, c)]
                for d in range(1, n1):
                    first_in[w][d, e].wait_recv()
                    tot = tot + land[d - 1, e]
                if e:
                    w2[e - 1] = tot
                    second_in[w].append((e, put(w2.at[e - 1], l2.at[e - 1], to[e])))
                else:
                    sums[w] = tot
    for w, at, n in ((0, 0, ca), (1, ca, cb)):
        tot = sums[w]
        for e, cp in second_in[w]:
            cp.wait_recv()
            tot = tot + parts[w][11][e - 1]
        zc[at:at + n] = tot
    for d in range(1, nz):
        pl.when(mz + d < nz)(functools.partial(pl.semaphore_wait, up.at[d], 1))
    quarter = lax.rem(mz, nq)
    in_z = [put(zc.at[pl.ds((zn * lax.rem(zs[d], nq)) // nq, zsize)], lz.at[mz], zdev[d]) for d in far_first(nz)[:-1]]
    lz[mz] = zc[pl.ds((zn * quarter) // nq, zsize)]
    for cp in in_z:
        cp.wait_recv()
    tot = lz[0]
    for z in range(1, nz):
        tot = tot + lz[z]
    zg[quarter] = tot
    done = 0
    if nq == 4:
        far = lax.rem(mz + 2 + 4 * lax.rem(mz, 2), nz)
        targets_z = (dev(far, my, mx, core), zdev[1], zdev[nz - 1])
        done = list(copies) + asks + reps
        in_z = [put(zg.at[quarter], zg.at[quarter], to) for to in targets_z]
        for cp in done:
            cp.wait_send()
        done = len(copies) - 3
        for cp in in_z:
            cp.wait_recv()
    base = [mine + p[4] + p[1][0] * p[3] for p in parts]
    spots = [base[w] + p[6][0] * p[8] for w, p in enumerate(parts)]
    for q in range(nq):
        lo = (zn * q) // nq
        end = (zn * (q + 1)) // nq
        for t in range(lo, end):
            at = spots[0] + t if t < ca else spots[1] + (t - ca)
            r_ref[pl.ds(at, 1)] = zg[q, t - lo:t - lo + 1]
    back = []

    def spread(w, at):
        n1, _, to, _, _, _, _, _, c, _, _, _ = parts[w]
        got = {d: put(r_ref.at[pl.ds(at, c)], r_ref.at[pl.ds(at, c)], to[d]) for d in far_first(n1)[:-1]}
        back.append(put(r_ref.at[pl.ds(at, c)], r_ref.at[pl.ds(at, c)], mate))
        return got

    second_in = [{}, {}]
    for w, p in enumerate(parts):
        for e in far_first(p[5])[:-1]:
            second_in[w][e] = (put(r_ref.at[pl.ds(spots[w], p[8])], r_ref.at[pl.ds(spots[w], p[8])], p[7][e]))
    first_in = [[spread(w, spots[w])] for w in range(2)]
    for i in range(max(nx, ny)):
        for w, (n1, own, _, n, off, n2, sub, _, c, _, _, _) in enumerate(parts):
            if i < n2 - 1:
                e = far_first(n2)[n2 - 2 - i]
                second_in[w][e].wait_recv()
                first_in[w].append(spread(w, base[w] + sub[n2 - e] * c))
    for cp in copies[done:] + ([] if done else asks + reps):
        cp.wait_send()
    sent = len(copies)
    for i in range(max(nx, ny)):
        for w, (n1, own, _, n, off, n2, sub, _, c, _, _, _) in enumerate(parts):
            if i < n2:
                e = far_first(n2)[n2 - 1 - i]
                for d in reversed(far_first(n1)[:-1]):
                    first_in[w][i][d].wait_recv()
                    at = mine + off + own[n1 - d] * n + sub[(n2 - e) % n2] * c
                    back.append(put(r_ref.at[pl.ds(at, c)], r_ref.at[pl.ds(at, c)], mate))
    for cp in back:
        cp.wait_recv()
    for cp in copies[sent:]:
        cp.wait_send()


def copy_count(group):
    nx, ny, nz = dims_of(group)
    return nx + ny + 2 * ((nx - 1) * ny + (ny - 1) * nx + nx - 1 + ny - 1) + nz - 1 + (3 if nz == 8 else 0) + 2 * nx * ny


def output_kernel(scale, r_ref, loss_ref, s1_hbm, n1_hbm, s2_hbm, n2_hbm, s1, n1, s2, n2, sem):
    at, k = 0, 0
    classes = s2.shape[0]
    copies = []
    for ref, hbm in ((s1, s1_hbm), (n1, n1_hbm), (s2, s2_hbm), (n2, n2_hbm)):
        rows, cols = ref.shape
        n = -(-rows // 8)
        step = n if n < 16 else 19
        for r0 in range(0, n, step):
            lo, hi = r0 * 8, min(rows, (r0 + step) * 8)
            for c in range(cols // 128):
                val = r_ref[at + c * n + r0:at + c * n + r0 + step].reshape(step * 8, 128)
                ref[lo:hi, c * 128:(c + 1) * 128] = val[0:hi - lo]
                if ref is s2 and c == 0:
                    loss_ref[...] = val[classes:classes + 1, 0:1] * scale
            cp = pltpu.make_async_copy(ref.at[lo:hi], hbm.at[lo:hi], sem.at[k])
            cp.start()
            copies.append(cp)
            k += 1
        at += n * (cols // 128)
    for cp in copies:
        cp.wait()


def solution(mesh):
    group = mesh.shape['g']

    def device_step(x_local, front_ids, nbr_one, nbr_two, labels, w_self1, w_nbr1, w_self2, w_nbr2):
        store, feat = x_local.shape
        targets, fan_one = nbr_one.shape
        seeds, fan_two = nbr_two.shape
        hidden, classes = w_self2.shape
        frows = -(-feat // 32) * 32
        scale = 1.0 / (group * seeds)
        fid = front_ids.reshape(-1, 128)
        width = -(-(store + 2 * HALO) // (FIELDS * 16)) * 16
        nx, ny, nz = dims_of(group)
        ca, cb = chunks_of(group)
        cx, cy, zn = ny * ca, nx * cb, ca + cb
        nq = max(1, nz // 2)
        zsize = -(-zn // nq)
        half = nx * cx + ny * cy
        total = 2 * half
        n = copy_count(group)
        dma = pltpu.SemaphoreType.DMA

        def buf(*lead):
            return VMEM((*lead, 8, 128), F32)

        vm, hbm = pl.BlockSpec(memory_space=VMEM), pl.BlockSpec(memory_space=pl.ANY)
        sums = pl.pallas_call(
            functools.partial(step_kernel, group, scale),
            name='train_step',
            out_shape=VMEM((total, 8, 128), F32),
            in_specs=[hbm] * 9,
            out_specs=vm,
            scratch_shapes=[
                VMEM(fid.shape, I32), VMEM((feat, store), BF16), VMEM((fan_one, targets), I32), VMEM((fan_two, seeds), I32),
                VMEM((1, seeds), I32), VMEM((feat, hidden), BF16), VMEM((feat, hidden), BF16), VMEM((classes, hidden), BF16),
                VMEM((classes, hidden), BF16), dma((9,)),
                VMEM((hidden, feat), BF16), VMEM((hidden, feat), BF16), VMEM((hidden, classes), BF16), VMEM((hidden, classes), BF16),
                VMEM((8, 128), I32), VMEM((2, 8, 128), I32), VMEM((2, frows // 2, 128), BF16),
                VMEM((2, frows // 2, 128), BF16), dma((8,)), dma((8,)),
                pltpu.SemaphoreType.REGULAR((nz,)),
                VMEM((16, 128), I32), VMEM((2, -(-fan_one // 8) * 8, targets), I32), VMEM((width, targets), I32),
                VMEM((FIELDS * width, 2 * targets), BF16), VMEM((feat, 2 * targets), F32), VMEM((hidden, targets), F32),
                VMEM((-(-classes // 16) * 16, 128), F32), buf(total),
                buf(half), buf(half), buf(nx - 1, ny, ca), buf(ny - 1, nx, cb), buf(ny - 1, ca), buf(nx - 1, cb),
                buf(ny - 1, ca), buf(nx - 1, cb), buf(zn), buf(nz, zsize), buf(nq, zsize),
                dma((n,)), dma((n,))],
            compiler_params=pltpu.CompilerParams(collective_id=0, has_side_effects=True,
                                                 vmem_limit_bytes=60 * 1024 * 1024),
        )(fid, x_local.T, nbr_one.T, nbr_two.T, labels.reshape(1, -1), w_self1, w_nbr1, w_self2.T, w_nbr2.T)
        loss, d_s1, d_n1, d_s2, d_n2 = pl.pallas_call(
            functools.partial(output_kernel, scale),
            name='split_outputs',
            out_shape=[jax.ShapeDtypeStruct((1, 1), F32), jax.ShapeDtypeStruct((feat, hidden), F32),
                       jax.ShapeDtypeStruct((feat, hidden), F32), jax.ShapeDtypeStruct((classes, hidden), F32),
                       jax.ShapeDtypeStruct((classes, hidden), F32)],
            in_specs=[vm], out_specs=[vm] + [hbm] * 4,
            scratch_shapes=[VMEM((feat, hidden), F32), VMEM((feat, hidden), F32), VMEM((classes, hidden), F32),
                            VMEM((classes, hidden), F32), dma((10,))],
        )(pltpu.with_memory_space_constraint(sums, VMEM))
        return loss[0, 0], d_s1, d_n1, d_s2.T, d_n2.T

    return jax.shard_map(device_step, mesh=mesh,
                         in_specs=(P('g', None), P('g'), P('g', None), P('g', None), P('g'), P(), P(), P(), P()),
                         out_specs=(P(), P(), P(), P(), P()), check_vma=False)
```
